128 devices in a mesh: dp: 16 (over z, y), tp: 8 (over x, core).
Axes of the slice: x: 4, y: 4, z: 4, core: 2. Of those that a mesh axis runs over, the one named last changes fastest.
Arguments:
- hidden: bfloat16 [2048, 128, 768], P('dp')
- positions: int32 [2048, 20], P('dp')
- labels: int32 [2048, 20], P('dp')
- weights: float32 [2048, 20], P('dp')
- w_t: bfloat16 [768, 768], replicated
- b_t: float32 [768], replicated
- gamma: float32 [768], replicated
- beta: float32 [768], replicated
- embed: bfloat16 [30592, 768], P('tp')
- out_bias: float32 [30592], P('tp')
Outputs:
- output 1: float32 [], replicated
- output 2: bfloat16 [2048, 128, 768], P('dp')
- output 3: float32 [768, 768], replicated
- output 4: float32 [768], replicated
- output 5: float32 [768], replicated
- output 6: float32 [768], replicated
- output 7: float32 [30592, 768], P('tp')
- output 8: float32 [30592], P('tp')
All inputs are finite; a program needn't handle non-finite values.
Results may differ from the reference program's by a relative error of at most 0.001.
Values sent between devices are 32-bit elements.
A program may use at most 1 GiB of HBM per device.

```python
import jax
import jax.numpy as jnp
from jax import lax

HIDDEN = 768
VOCAB_REAL = 30522
VOCAB_PAD = 30592
SEQ_LEN = 128
MAX_PRED = 20
BATCH_TOTAL = 2048
BLOCK_SEQ = 8
NUM_BLOCKS = BATCH_TOTAL // BLOCK_SEQ
BLOCK_ROWS = BLOCK_SEQ * MAX_PRED
LN_EPS = 1e-12
LOSS_EPS = 1e-5


def setup_inputs(seed: int = 0) -> dict:
    key = jax.random.key(seed)
    keys = jax.random.split(key, 10)
    hidden = jax.random.normal(keys[0], (BATCH_TOTAL, SEQ_LEN, HIDDEN), jnp.float32).astype(jnp.bfloat16)
    row_keys = jax.random.split(keys[1], BATCH_TOTAL)
    positions = jax.vmap(lambda row_key: jax.random.permutation(row_key, SEQ_LEN)[:MAX_PRED])(row_keys).astype(jnp.int32)
    labels = jax.random.randint(keys[2], (BATCH_TOTAL, MAX_PRED), 0, VOCAB_REAL, dtype=jnp.int32)
    pred_counts = jax.random.randint(keys[3], (BATCH_TOTAL,), 1, MAX_PRED + 1, dtype=jnp.int32).at[0].set(MAX_PRED)
    weights = (jnp.arange(MAX_PRED, dtype=jnp.int32)[None, :] < pred_counts[:, None]).astype(jnp.float32)
    w_t = (jax.random.normal(keys[4], (HIDDEN, HIDDEN), jnp.float32) * HIDDEN ** -0.5).astype(jnp.bfloat16)
    b_t = 0.5 * jax.random.normal(keys[5], (HIDDEN,), jnp.float32)
    gamma = 1.0 + 0.3 * jax.random.normal(keys[6], (HIDDEN,), jnp.float32)
    beta = 0.3 * jax.random.normal(keys[7], (HIDDEN,), jnp.float32)
    embed = (jax.random.normal(keys[8], (VOCAB_PAD, HIDDEN), jnp.float32) * (1.5 * HIDDEN ** -0.5)).astype(jnp.bfloat16)
    raw_bias = 0.5 * jax.random.normal(keys[9], (VOCAB_PAD,), jnp.float32)
    out_bias = jnp.where(jnp.arange(VOCAB_PAD) < VOCAB_REAL, raw_bias, -1e9)
    return {"hidden": hidden, "positions": positions, "labels": labels, "weights": weights, "w_t": w_t, "b_t": b_t, "gamma": gamma, "beta": beta, "embed": embed, "out_bias": out_bias}


def gelu_norm(pre_act, gamma, beta):
    activated = jax.nn.gelu(pre_act, approximate=False)
    mean_val = jnp.mean(activated, axis=-1, keepdims=True)
    centered = activated - mean_val
    variance = jnp.mean(centered * centered, axis=-1, keepdims=True)
    return centered * lax.rsqrt(variance + LN_EPS) * gamma + beta


def reference(hidden, positions, labels, weights, w_t, b_t, gamma, beta, embed, out_bias):
    picked = jnp.take_along_axis(hidden, positions[:, :, None], axis=1)
    tok_rows = picked.reshape(BATCH_TOTAL * MAX_PRED, HIDDEN)
    pre_act = jnp.dot(tok_rows, w_t, preferred_element_type=jnp.float32) + b_t
    normed, norm_vjp = jax.vjp(gelu_norm, pre_act, gamma, beta)
    t_bf = normed.astype(jnp.bfloat16)
    flat_w = weights.reshape(-1)
    denom = jnp.sum(flat_w) + LOSS_EPS
    vocab_ids = jnp.arange(VOCAB_PAD, dtype=jnp.int32)

    def block_step(carry, block):
        d_embed, d_bias, loss_sum = carry
        t_blk, lab_blk, w_blk = block
        logits = jnp.dot(t_blk, embed.T, preferred_element_type=jnp.float32) + out_bias
        row_max = jnp.max(logits, axis=1)
        shifted = jnp.exp(logits - row_max[:, None])
        sum_exp = jnp.sum(shifted, axis=1)
        log_norm = jnp.log(sum_exp) + row_max
        lab_hot = lab_blk[:, None] == vocab_ids[None, :]
        target_logit = jnp.sum(jnp.where(lab_hot, logits, 0.0), axis=1)
        soft_probs = shifted * (1.0 / sum_exp)[:, None]
        d_logits = jnp.where(lab_hot, soft_probs - 1.0, soft_probs) * (w_blk / denom)[:, None]
        dz_bf = d_logits.astype(jnp.bfloat16)
        d_embed = d_embed + jnp.dot(dz_bf.T, t_blk, preferred_element_type=jnp.float32)
        d_bias = d_bias + jnp.sum(d_logits, axis=0)
        loss_sum = loss_sum + jnp.sum(w_blk * (log_norm - target_logit))
        d_normed = jnp.dot(dz_bf, embed, preferred_element_type=jnp.float32)
        return (d_embed, d_bias, loss_sum), d_normed

    init = (jnp.zeros((VOCAB_PAD, HIDDEN), jnp.float32), jnp.zeros((VOCAB_PAD,), jnp.float32), jnp.zeros((), jnp.float32))
    blocks = (t_bf.reshape(NUM_BLOCKS, BLOCK_ROWS, HIDDEN), labels.reshape(NUM_BLOCKS, BLOCK_ROWS), flat_w.reshape(NUM_BLOCKS, BLOCK_ROWS))
    (d_embed, d_out_bias, loss_sum), d_normed = lax.scan(block_step, init, blocks)
    loss = loss_sum / denom
    d_pre, d_gamma, d_beta = norm_vjp(d_normed.reshape(BATCH_TOTAL * MAX_PRED, HIDDEN))
    d_pre_bf = d_pre.astype(jnp.bfloat16)
    d_w_t = jnp.dot(tok_rows.T, d_pre_bf, preferred_element_type=jnp.float32)
    d_b_t = jnp.sum(d_pre, axis=0)
    d_rows = jnp.dot(d_pre_bf, w_t.T, preferred_element_type=jnp.float32).astype(jnp.bfloat16)
    row_ids = jnp.arange(BATCH_TOTAL)[:, None]
    d_hidden = jnp.zeros((BATCH_TOTAL, SEQ_LEN, HIDDEN), jnp.bfloat16).at[row_ids, positions].add(d_rows.reshape(BATCH_TOTAL, MAX_PRED, HIDDEN))
    return (loss, d_hidden, d_w_t, d_b_t, d_gamma, d_beta, d_embed, d_out_bias)
```

```python
import functools

import jax
import jax.numpy as jnp
from jax import lax
from jax.experimental import pallas as pl
from jax.experimental.pallas import tpu as pltpu
from jax.sharding import PartitionSpec as P

F32 = jnp.float32
BF16 = jnp.bfloat16
I32 = jnp.int32
LN_EPS = 1e-12
LOSS_EPS = 1e-5
RSQRT2 = 0.7071067811865476
PAD_BIAS = -3e38
GB = 8
NT = 5
NBUF = 4
VMEM_MAX = 67043328
NCH = 8
NN = (((1,), (0,)), ((), ()))
NTR = (((1,), (1,)), ((), ()))
TN = (((0,), (0,)), ((), ()))


def mm(a, b, dims=NN):
    return lax.dot_general(a, b, dims, preferred_element_type=F32)


LANES = 128
ALL = None
ROWS, COLS = ({"axis": i, "keepdims": True} for i in range(2))
LAB, LIVE, SRC, MAX, SUM, TGT = (slice(i, i + 1) for i in range(6))


class Dims:
    def __init__(self, hidden, positions, embed):
        self.B, self.L, self.D = hidden
        self.P = positions[1]
        self.V = embed[0]
        self.G = self.B // GB
        self.S = GB * self.P
        self.N = self.B * self.P
        self.TT = self.N // NT
        self.BLK = -(-self.V // LANES) * GB
        self.VP = 16 * self.BLK
        self.CH = 2 * self.BLK
        self.NR = self.N // 8
        self.HN, self.HD, self.HB, self.HR = self.N // 2, self.D // 2, self.BLK // 2, self.NR // 2
        self.WR = self.D // 8
        self.WP = self.WR // 4
        self.CL = -(-self.CH // LANES) * LANES


def cuts(n):
    return [slice(i, min(i + LANES, n)) for i in range(0, n, LANES)]


def row_of(ref):
    return jnp.concatenate([ref[slice(i, i + 1), :] for i in range(ref.shape[0])], axis=1)


def forward_kernel(d, h_hbm, idx_ref, lab_ref, w_ref, wt_ref, bt_ref, gm_ref, be_ref, e_hbm, bias_ref,
                   h_out, t_out, z_out, meta_out, col_out, e_out, cnt_out,
                   hin, hb, tb, ub, eb, bcol, zb, col, meta, keys, cntv, cnt, par3, hsem, esem, zsem, osem):
    rows_g = GB * d.L
    tail = d.V - (NCH - 1) * d.CH

    def h_copy(g, slot):
        return pltpu.make_async_copy(h_hbm.at[pl.ds(g * rows_g, rows_g)], hin.at[slot], hsem.at[slot])

    def e_copy(c):
        n = d.CH if c < NCH - 1 else tail
        return pltpu.make_async_copy(e_hbm.at[pl.ds(c * d.CH, n)], eb.at[pl.ds(c * d.CH, n)], esem.at[c])

    for g in range(NBUF):
        h_copy(g, g).start()
    for c in range(NCH):
        e_copy(c).start()

    cntv[...] = jnp.broadcast_to(jnp.sum(w_ref[...], **ROWS), cntv.shape).astype(I32)
    to_smem = pltpu.make_async_copy(cntv, cnt, osem.at[5])
    to_smem.start()
    outs = [pltpu.make_async_copy(a, b, osem.at[i])
            for i, (a, b) in enumerate(((hb, h_out), (col, col_out), (eb, e_out), (tb, t_out), (meta, meta_out)))]
    outs.append(pltpu.make_async_copy(cntv, cnt_out, osem.at[6]))
    outs[5].start()

    key = lab_ref[...] * 2048 + idx_ref[...] + 1
    keys[...] = jnp.concatenate([key, jnp.zeros((LANES - d.P, d.B), I32)], axis=0).T
    for i, ref in enumerate((bt_ref, gm_ref, be_ref)):
        par3[slice(i, i + 1), :] = row_of(ref)
    hb[...] = jnp.zeros_like(hb)
    tb[...] = jnp.zeros_like(tb)
    col[...] = jnp.zeros_like(col)
    if tail < d.CH:
        eb[d.V:, :] = jnp.zeros((d.VP - d.V, d.D), BF16)
    one_row = lax.broadcasted_iota(I32, (8, d.TT), 0) == 4
    for n in range(NT):
        meta[n] = jnp.where(one_row, 1.0, 0.0)
    for i, rows in enumerate(cuts(d.VP)):
        bcol[rows, :] = jnp.broadcast_to(bias_ref[slice(i, i + 1), :], (LANES, LANES)).T
    to_smem.wait()

    lane = lax.broadcasted_iota(I32, (1, LANES), 1)
    r_iota = lax.broadcasted_iota(I32, (d.S, LANES), 0)
    p_iota = lax.broadcasted_iota(I32, (1, LANES), 1)
    src_iota = lax.broadcasted_iota(I32, (d.S, rows_g), 1)

    def group(g, o):
        slot = lax.rem(g, NBUF)
        off = jnp.int32(0)
        key = jnp.zeros((d.S, LANES), I32)
        for j in range(GB):
            b = g * GB + j
            n_j = cnt[0, b]
            rank = jnp.where(p_iota < n_j, p_iota + off, -1)
            key = key + jnp.where(r_iota == rank, keys[pl.ds(b, 1), :] + j * d.L, 0)
            off = off + n_j
        src = jnp.sum((key & 2047).astype(F32), **COLS)
        lab = jnp.sum((key >> 11).astype(F32), **COLS)
        hot = (src_iota == src.astype(I32) - 1).astype(BF16)
        h_copy(g, slot).wait()
        o = pl.multiple_of(o, 16)
        hb[pl.ds(o, d.S), :] = mm(hot, hin[slot]).astype(BF16)
        live = (src > 0).astype(F32)
        col[pl.ds(o, d.S), :] = jnp.where(lane == 0, lab, jnp.where(lane == 1, live, src - 1))

        @pl.when(g + NBUF < d.G)
        def _():
            h_copy(g + NBUF, slot).start()

        return o + ((off + 15) // 16) * 16

    used = lax.fori_loop(0, d.G, group, jnp.int32(0))
    tiles = (used + d.TT - 1) // d.TT
    outs[0].start()
    outs[1].start()
    for c in range(NCH):
        e_copy(c).wait()
    outs[2].start()

    base_v = lax.axis_index("tp") * d.V
    sub = lax.broadcasted_iota(I32, (8, d.TT), 0)
    rb = min(128, d.TT)

    def z_copy(n, c):
        return pltpu.make_async_copy(zb.at[lax.rem(n, 2), c], z_out.at[n, pl.ds(c * d.CH, d.CH)],
                                     zsem.at[lax.rem(n, 2), c])

    def tile(n, carry):
        par = lax.rem(n, 2)
        base = pl.multiple_of(n * d.TT, d.TT)

        @pl.when(n >= 2)
        def _():
            for c in range(NCH):
                z_copy(n, c).wait()

        ub[...] = mm(hb[pl.ds(base, d.TT), :], wt_ref[...]) + par3[LAB, :]

        def norm(i, carry):
            r = pl.multiple_of(i * rb, rb)
            u = ub[pl.ds(r, rb), :]
            a = 0.5 * u * (1.0 + lax.erf(u * RSQRT2))
            ctr = a - jnp.mean(a, **COLS)
            var = jnp.mean(ctr * ctr, **COLS)
            t = ctr * lax.rsqrt(var + LN_EPS) * par3[LIVE, :] + par3[SRC, :]
            tb[pl.ds(base + r, rb), :] = t.astype(BF16)
            return carry

        lax.fori_loop(0, d.TT // rb, norm, 0)
        for cols in cuts(d.TT):
            blk = col[pl.ds(base + cols.start, LANES), :].T
            meta[n, :3, cols] = blk[:3, :]

        t_n = tb[pl.ds(base, d.TT), :]
        lab = meta[n, LAB, :].astype(I32) - base_v
        lab8 = jnp.broadcast_to(jnp.where(lab < d.V, lab, -1), (8, d.TT))
        m8 = jnp.full((8, d.TT), -jnp.inf, F32)
        s8 = jnp.zeros((8, d.TT), F32)
        t8 = jnp.zeros((8, d.TT), F32)
        reps = d.TT // LANES

        def product(c):
            z = mm(eb[c * d.CH:(c + 1) * d.CH, :], t_n, NTR)
            b = bcol[c * d.CH:(c + 1) * d.CH, :]
            z = z + jnp.concatenate([b] * reps, axis=1)
            zb[par, c] = z
            mx = jnp.max(z.reshape(d.CH // 8, 8, d.TT), axis=0)
            return jnp.broadcast_to(jnp.max(mx, **ROWS), (8, d.TT))

        nxt = product(0)
        for c in range(NCH):
            z_copy(n, c).start()
            mx = jnp.maximum(m8, nxt)
            if c + 1 < NCH:
                nxt = product(c + 1)
            s8 = s8 * jnp.exp(m8 - mx)
            m8 = mx
            for i in range(d.CH // 8):
                zz = zb[par, c, i * 8:(i + 1) * 8, :]
                s8 = s8 + jnp.exp(zz - m8)
                t8 = t8 + jnp.where(sub + (c * d.CH + i * 8) == lab8, zz, 0.0)
        meta[n, MAX, :] = m8[LAB, :]
        meta[n, SUM, :] = jnp.sum(s8, **ROWS)
        meta[n, TGT, :] = jnp.sum(t8, **ROWS)
        return carry

    lax.fori_loop(0, tiles, tile, 0)
    outs[3].start()
    outs[4].start()

    def drain(n, carry):
        for c in range(NCH):
            z_copy(n, c).wait()
        return carry

    lax.fori_loop(jnp.maximum(tiles - 2, 0), tiles, drain, 0)
    for cp in outs:
        cp.wait()


def forward(d, h2, idx, lab, w, w_t, bt, gm, be, embed, bias):
    any_ = pl.BlockSpec(memory_space=pl.ANY)
    vm = pl.BlockSpec(memory_space=pltpu.VMEM)
    sd = jax.ShapeDtypeStruct
    dma = pltpu.SemaphoreType.DMA
    return pl.pallas_call(
        functools.partial(forward_kernel, d),
        out_shape=(sd((d.N, d.D), BF16), sd((d.N, d.D), BF16), sd((NT, d.VP, d.TT), F32), sd((NT, 8, d.TT), F32),
                   sd((d.N, LANES), F32), sd((d.VP, d.D), BF16), sd((8, d.B), I32)),
        in_specs=[any_, vm, vm, vm, vm, vm, vm, vm, any_, vm],
        out_specs=(any_,) * 7,
        scratch_shapes=[
            pltpu.VMEM((NBUF, GB * d.L, d.D), BF16),
            pltpu.VMEM((d.N, d.D), BF16),
            pltpu.VMEM((d.N, d.D), BF16),
            pltpu.VMEM((d.TT, d.D), F32),
            pltpu.VMEM((d.VP, d.D), BF16),
            pltpu.VMEM((d.VP, LANES), F32),
            pltpu.VMEM((2, NCH, d.CH, d.TT), F32),
            pltpu.VMEM((d.N, LANES), F32),
            pltpu.VMEM((NT, 8, d.TT), F32),
            pltpu.VMEM((d.B, LANES), I32),
            pltpu.VMEM((8, d.B), I32),
            pltpu.SMEM((8, d.B), I32),
            pltpu.VMEM((8, d.D), F32),
            dma((NBUF,)), dma((NCH,)), dma((2, NCH)), dma((7,)),
        ],
        compiler_params=pltpu.CompilerParams(vmem_limit_bytes=VMEM_MAX),
        name="mlm_forward",
    )(h2, idx, lab, w, w_t, bt, gm, be, embed, bias)


MESH = pl.DeviceIdType.MESH
RING = (1, 2, 3)
NSEM = 128
ORDER = ((2, 0), (2, 1), (1, 1), (3, 0), (1, 0), (3, 1), (0, 0), (0, 1))
FINISH = (0, 3, 1, 2)


def train_kernel(d, t_hbm, h_hbm, z_hbm, meta, e_hbm, wt_ref, bt_ref, gm_ref, be_ref,
                 de_out, dh_out, dwt_out, vec_out, dbo_out,
                 tb, eb, zb, dzb, dt, de, fm, fp, r2a, r2b, f2m, f2p, dr, xa, xb, xm, xp,
                 ub, dub, hown, wr, wxa, wxb, wxm, wxp, wp, wq, wag, srecv, comb, dacc, vb, vby, vbz,
                 dnp, dnq, vec, vect, vecy, vecz, lsem, esem, zsem, osem, ss, rs):
    dp = lax.axis_index("dp")
    tp = lax.axis_index("tp")
    zc, yc = dp // 4, lax.rem(dp, 4)
    x, core = tp // 2, lax.rem(tp, 2)
    other = 1 - core
    pm, qm = 1 + 3 * core, 4 - 3 * core
    p = yc + core * (zc - yc)
    q = zc + core * (yc - zc)
    N, D, CH, BLK, TT, NR = d.N, d.D, d.CH, d.BLK, d.TT, d.NR
    HN, HD, WR, WP = d.HN, d.HD, d.WR, d.WP

    def rem4(v):
        return lax.rem(v + 4, 4)

    def rem8(v):
        return lax.rem(v + 8, 8)

    def at_p(r):
        return {"dp": rem4(p + r) * pm + q * qm}

    def at_q(r):
        return {"dp": p * pm + rem4(q + r) * qm}

    def at_y(r):
        return {"dp": zc * 4 + rem4(yc + r)}

    def at_z(r):
        return {"dp": rem4(zc + r) * 4 + yc}

    def at_x(r):
        return {"tp": rem4(x + r) * 2 + core}

    def at_t(r):
        return {"tp": rem8(tp + r)}

    sib = {"tp": x * 2 + other}

    def al(v, m=8):
        return pl.multiple_of(v, m)

    listed = []

    def link(src, dst, dev):
        i = len(listed)
        listed.append(pltpu.make_async_remote_copy(src_ref=src, dst_ref=dst, send_sem=ss.at[i], recv_sem=rs.at[i],
                                                   device_id=dev, device_id_type=MESH))
        return i

    def send(src, dst, dev):
        i = link(src, dst, dev)
        listed[i].start()
        return i

    def got(dst, i):
        pltpu.make_async_remote_copy(src_ref=dst, dst_ref=dst, send_sem=ss.at[i], recv_sem=rs.at[i],
                                     device_id=sib, device_id_type=MESH).wait_recv()

    def share(buf, own, at):
        return [send(buf.at[own], buf.at[own], at(r)) for r in RING]

    def shared(buf, own, ids):
        for r, i in zip(RING, ids):
            got(buf.at[rem4(own - r)], i)
        return buf[0] + buf[1] + buf[2] + buf[3]

    def half(ref, h):
        n = ref.shape[0] // 2
        return ref.at[pl.ds(h * n, n)]

    def add(dst, srcs):
        nr = dst.shape[0]
        step = max(s for s in (8, 24, 40) if nr % s == 0)

        def body(i, carry):
            rows = pl.ds(al(i * step), step)
            v = dst[rows, :]
            for s in srcs:
                v = v + s[rows, :]
            dst[rows, :] = v
            return carry

        lax.fori_loop(0, nr // step, body, 0)

    class Scatter:
        def __init__(self, blk, a, b, m, pp, at):
            self.blk, self.a, self.b, self.m, self.pp, self.at = blk, a, b, m, pp, at

        def begin(self):
            blk, at = self.blk, self.at
            self.ids = [send(blk(2, 0), self.a, at(1)), send(blk(2, 1), self.b, at(3)),
                        send(blk(1, 1), half(self.m, 1), at(1)), send(blk(3, 0), half(self.pp, 0), at(3))]

        def middle(self):
            blk, at = self.blk, self.at
            got(self.a, self.ids[0])
            add(blk(1, 0), [self.a])
            self.ids.append(send(blk(1, 0), half(self.m, 0), at(1)))
            got(self.b, self.ids[1])
            add(blk(3, 1), [self.b])
            self.ids.append(send(blk(3, 1), half(self.pp, 1), at(3)))

        def end(self):
            ids = self.ids
            got(half(self.m, 1), ids[2])
            got(half(self.pp, 0), ids[3])
            got(half(self.m, 0), ids[4])
            got(half(self.pp, 1), ids[5])

    class Gather:
        def __init__(self, row, at, to_sib=None):
            self.row, self.at, self.to_sib, self.sib_ids = row, at, to_sib, []

        def pass_on(self, r, src=None):
            if self.to_sib is not None:
                src = self.row(r) if src is None else src
                self.sib_ids.append((r, send(src, self.row(r), sib)))

        def begin(self, src):
            self.ids = [send(src, self.row(0), self.at(1)), send(src, self.row(0), self.at(3))]
            self.pass_on(0, src)

        def middle(self):
            got(self.row(3), self.ids[0])
            self.ids.append(send(self.row(3, 0), self.row(3, 0), self.at(1)))
            self.pass_on(3)
            got(self.row(1), self.ids[1])
            self.ids.append(send(self.row(1, 1), self.row(1, 1), self.at(3)))
            self.pass_on(1)

        def end(self):
            got(self.row(2, 0), self.ids[2])
            got(self.row(2, 1), self.ids[3])
            self.pass_on(2)

        def close(self):
            for r, i in self.sib_ids:
                got(self.to_sib(r), i)

    def spot(ref, base, n, h=ALL):
        if h is ALL:
            return ref.at[pl.ds(al(base), n)]
        return ref.at[pl.ds(al(base + h * (n // 2)), n // 2)]

    def chunk_id(k):
        out = p * 0
        for i, (rel, h) in enumerate(ORDER):
            out = jnp.where(k == i, rem4(p + rel) * 2 + h, out)
        return out

    def is_dt(s):
        return (s >= 4) & (s < 12)

    def chunk_at(s):
        return jnp.where(is_dt(s), s - 4, chunk_id(jnp.where(s < 4, s, s - 8)))

    def loads(s):
        slot = lax.rem(s, 2)
        r = chunk_at(s) * CH
        return [pltpu.make_async_copy(e_hbm.at[pl.ds(al(r, 16), CH)], eb.at[slot], esem.at[slot])] + [
            pltpu.make_async_copy(z_hbm.at[n, pl.ds(al(r), CH)], zb.at[slot, n], zsem.at[slot, n]) for n in range(NT)]

    t_load = pltpu.make_async_copy(t_hbm, tb, lsem.at[0])
    h_load = pltpu.make_async_copy(h_hbm.at[pl.ds(al((core * 4 + x) * NR, 16), NR)], hown, lsem.at[1])
    for cp in loads(jnp.int32(0)):
        cp.start()
    t_load.start()
    h_load.start()

    barrier = pltpu.get_barrier_semaphore()
    peers = [f(r) for f in (at_y, at_z) for r in RING] + [at_t(r) for r in range(1, 8)]
    for dev in peers:
        pl.semaphore_signal(barrier, inc=1, device_id=dev, device_id_type=MESH)
    wsum = jnp.zeros((1, 1), F32)
    for n in range(NT):
        wsum = wsum + jnp.sum(meta[n, LIVE, :], **COLS)
    dnp[yc] = jnp.broadcast_to(wsum, dnp.shape[1:])
    srecv[tp] = meta[...]
    pl.semaphore_wait(barrier, len(peers))

    ids_y = share(dnp, yc, at_y)
    ids_t = [send(meta, srecv.at[tp], at_t(r)) for r in range(1, 8)]
    dt[...] = jnp.zeros_like(dt)
    for k in (0, 2, 4, 6, 12, 14):
        de[k:k + 2] = jnp.zeros((2, BLK, D), F32)
    vb[...] = jnp.zeros_like(vb)
    dnq[zc] = shared(dnp, yc, ids_y)
    ids_z = share(dnq, zc, at_z)
    for r, i in zip(range(1, 8), ids_t):
        got(srecv.at[rem8(tp - r)], i)
    tiles = []
    for n in range(NT):
        mx = srecv[0, n, MAX, :]
        for k in range(1, 8):
            mx = jnp.maximum(mx, srecv[k, n, MAX, :])
        tot = jnp.zeros((1, TT), F32)
        tgt = jnp.zeros((1, TT), F32)
        for k in range(8):
            tot = tot + srecv[k, n, SUM, :] * jnp.exp(srecv[k, n, MAX, :] - mx)
            tgt = tgt + srecv[k, n, TGT, :]
        lab = meta[n, LAB, :] - (tp * d.V).astype(F32)
        comb[n, LAB, :] = mx
        comb[n, LIVE, :] = 1.0 / tot
        comb[n, MAX, :] = jnp.where(lab < d.V, lab, -1.0)
        tiles.append(jnp.log(tot) + mx - tgt)
    denom = shared(dnq, zc, ids_z)[LAB, LAB] + LOSS_EPS
    ce = jnp.zeros((1, TT), F32)
    for n in range(NT):
        w = meta[n, LIVE, :]
        c = w / denom
        comb[n, LIVE, :] = comb[n, LIVE, :] * c
        comb[n, SRC, :] = c
        ce = ce + w * tiles[n]
    ce = jnp.sum(ce, **COLS) / denom
    t_load.wait()

    sub = lax.broadcasted_iota(I32, (16, TT), 0)
    row8 = lax.broadcasted_iota(I32, (NCH, LANES), 0)
    dacc[CH:, :] = jnp.zeros((d.CL - CH, LANES), F32)

    def grads(slot, n, cid, sums):
        m8 = jnp.broadcast_to(comb[n, LAB, :], (16, TT))
        a8 = jnp.broadcast_to(comb[n, LIVE, :], (16, TT))
        c8 = jnp.broadcast_to(comb[n, SRC, :], (16, TT))
        l8 = jnp.broadcast_to(comb[n, MAX, :].astype(I32) - cid * CH, (16, TT))
        live = c8 > 0
        for i in range(CH // 16):
            rows = slice(i * 16, (i + 1) * 16)
            g = jnp.exp(zb[slot, n, rows, :] - m8) * a8
            g = g - jnp.where(sub + i * 16 == l8, c8, 0.0)
            g = jnp.where(live, g, 0.0)
            dzb[n % 2, rows, :] = g.astype(BF16)
            if sums:
                part = sum(g[:, cols] for cols in cuts(TT))
                dacc[rows, :] = part if n == 0 else dacc[rows, :] + part

    two = [de.at[pl.ds(2 * k, 2)] for k in range(8)]
    lo, hi = pl.ds(0, 2), pl.ds(2, 2)
    stage1 = [link(two[0], two[4], at_p(1)), link(two[1], two[5], at_p(3)),
              link(two[2], fm.at[hi], at_p(1)), link(two[3], fp.at[lo], at_p(3)),
              link(two[4], fm.at[lo], at_p(1)), link(two[5], fp.at[hi], at_p(3))]
    to_sib = link(dt.at[pl.ds(al(other * HN), HN)], dr, sib)

    def add2(dst, src):
        for b in range(2):
            add(dst.at[b], [src.at[b]])

    def xrow(r, h=ALL):
        return spot(dt, (core * 4 + rem4(x + r)) * NR, NR, h)

    rs_x = Scatter(xrow, xa, xb, xm, xp, at_x)

    def step(s, carry):
        slot = lax.rem(s, 2)
        for cp in loads(s):
            cp.wait()

        @pl.when(s < 15)
        def _():
            for cp in loads(s + 1):
                cp.start()

        cid = chunk_at(s)

        @pl.when(is_dt(s))
        def _():
            for n in range(NT):
                grads(slot, n, cid, False)
                dt[n * TT:(n + 1) * TT, :] += mm(dzb[n % 2], eb[slot], TN)

        @pl.when(s == 11)
        def _():
            listed[to_sib].start()

        @pl.when(jnp.logical_not(is_dt(s)))
        def _():
            k = jnp.where(s < 4, s, s - 8)
            for i in (0, 1):
                @pl.when(k == i + 4)
                def _(i=i):
                    got(two[i + 4], stage1[i])
            for n in range(NT):
                grads(slot, n, cid, True)
                prod = mm(dzb[n % 2], tb[n * TT:(n + 1) * TT, :]).reshape(2, BLK, D)
                de[pl.ds(2 * k, 2)] += prod
            for cols in cuts(d.CL):
                tot = jnp.broadcast_to(jnp.sum(dacc[cols, :].T, **ROWS), (NCH, LANES))
                vb[:NCH, cols] = jnp.where(row8 == cid, tot, vb[:NCH, cols])
            for i in range(6):
                @pl.when(k == i)
                def _(i=i):
                    listed[stage1[i]].start()

        return carry

    lax.fori_loop(0, 16, step, 0)

    got(dr, to_sib)
    add(dt.at[pl.ds(al(core * HN), HN)], [dr])
    rs_x.begin()
    own = de.at[pl.ds(12, 4)]
    got(fp.at[lo], stage1[3])
    add2(own.at[lo], fp.at[lo])
    got(fm.at[hi], stage1[2])
    add2(own.at[hi], fm.at[hi])
    vb[NCH:, :] = jnp.broadcast_to(ce, (NCH, d.CL))
    vby[yc] = vb[...]
    ids_y = share(vby, yc, at_y)
    h_load.wait()
    ub[...] = mm(hown[...], wt_ref[...]) + row_of(bt_ref)
    gamma = row_of(gm_ref)
    rs_x.middle()

    got(fm.at[lo], stage1[4])
    add2(own.at[lo], fm.at[lo])
    got(fp.at[hi], stage1[5])
    add2(own.at[hi], fp.at[hi])

    def ob(r, h=ALL):
        blk = own.at[rem4(q + r)]
        return blk if h is ALL else half(blk, h)

    rs_q = Scatter(ob, r2a, r2b, f2m, f2p, at_q)
    rs_q.begin()
    vbz[zc] = shared(vby, yc, ids_y)
    ids_z = share(vbz, zc, at_z)
    rs_q.middle()
    rs_q.end()
    fin = ob(0)
    add(fin, [f2m, f2p])

    def orow(rp, rq, h=ALL):
        return spot(de_out, (rem4(p + rp) * 4 + rem4(q + rq)) * BLK, BLK, h)

    ag_q = Gather(lambda r, h=ALL: orow(0, r, h), at_q)
    ag_q.begin(fin)
    keep = [pltpu.make_async_copy(fin, orow(0, 0), osem.at[0])]
    keep[0].start()
    ag_p = [Gather(lambda r, h=ALL, j=j: orow(r, j, h), at_p) for j in FINISH]

    rs_x.end()
    lb = 64 if NR % 64 == 0 else 16
    dtown = xrow(0)
    vec[...] = jnp.zeros_like(vec)

    def back(i, carry):
        rows = pl.ds(al(i * lb, 16), lb)
        u = ub[rows, :]
        cdf = 0.5 * (1.0 + lax.erf(u * RSQRT2))
        a = u * cdf
        ctr = a - jnp.mean(a, **COLS)
        rstd = lax.rsqrt(jnp.mean(ctr * ctr, **COLS) + LN_EPS)
        xh = ctr * rstd
        g = dtown[rows, :] + xm[rows, :] + xp[rows, :]
        gx = g * xh
        gg = g * gamma
        m1 = jnp.mean(gg, **COLS)
        m2 = jnp.mean(gg * xh, **COLS)
        da = rstd * (gg - m1 - xh * m2)
        pdf = jnp.exp(u * u * -0.5) * 0.3989422804014327
        du = da * (cdf + u * pdf)
        dub[rows, :] = du.astype(BF16)
        for j, v in enumerate((gx, g, du)):
            vec[j] += jnp.sum(v.reshape(lb // GB, GB, D), axis=0)
        return carry

    lax.fori_loop(0, NR // lb, back, 0)
    listed[to_sib].wait_send()
    dwt = dt.at[pl.ds(al(other * HN), D)]
    for cols in cuts(D):
        dwt[:, cols] = mm(hown[...], dub[:, cols], TN)
    i_wr = send(dwt.at[pl.ds(al(other * HD), HD)], wr, sib)
    ag_p[0].begin(fin)
    vect[tp] = jnp.concatenate([jnp.sum(vec[i], **ROWS) for i in range(GB)], axis=0)
    ids_t = [send(vect.at[tp], vect.at[tp], at_t(r)) for r in range(1, 8)]
    for cols in cuts(D):
        ub[:, cols] = mm(dub[...], wt_ref[cols, :], NTR).astype(BF16).astype(F32)

    def wrow(r, h=ALL):
        return spot(dwt, core * HD + rem4(x + r) * WR, WR, h)

    rs_w = Scatter(wrow, wxa, wxb, wxm, wxp, at_x)
    got(wr, i_wr)
    add(dwt.at[pl.ds(al(core * HD), HD)], [wr])
    rs_w.begin()
    ag_q.middle()
    ag_p[1].begin(orow(0, 3))
    ag_p[2].begin(orow(0, 1))
    rs_w.middle()

    def hrow(c):
        return lambda r, h=ALL: spot(dh_out, (c * 4 + rem4(x + r)) * NR, NR, h)

    ag_h = Gather(hrow(core), at_x, hrow(other))
    ag_h.begin(ub)
    keep.append(pltpu.make_async_copy(ub, hrow(core)(0), osem.at[1]))
    keep[1].start()

    for r, i in zip(range(1, 8), ids_t):
        got(vect.at[rem8(tp - r)], i)
    acc = vect[0]
    for k in range(1, 8):
        acc = acc + vect[k]
    vecy[yc] = acc
    ids_y = share(vecy, yc, at_y)

    rs_w.end()
    wown = wrow(0)
    add(wown, [wxm, wxp])

    def piece(ref, k):
        return ref.at[pl.ds(al(k * WP), WP)]

    ids_q = [send(piece(wown, rem4(q + r)), wq.at[q], at_q(r)) for r in RING]
    wq[q] = piece(wown, q)[...]
    ag_q.end()
    ag_p[3].begin(orow(0, 2))
    wp[p] = shared(wq, q, ids_q)
    ids_p = share(wp, p, at_p)
    ag_p[0].middle()
    dbo_out[...] = shared(vbz, zc, ids_z)
    vecz[zc] = shared(vecy, yc, ids_y)
    ids_z = share(vecz, zc, at_z)
    piece(wag, q)[...] = shared(wp, p, ids_p)
    ids_q = [send(piece(wag, q), piece(wag, q), at_q(r)) for r in RING]
    ag_p[1].middle()
    for r, i in zip(RING, ids_q):
        got(piece(wag, rem4(q - r)), i)

    def grow(c):
        return lambda r, h=ALL: spot(dwt_out, c * HD + rem4(x + r) * WR, WR, h)

    ag_w = Gather(grow(core), at_x, grow(other))
    ag_w.begin(wag)
    keep.append(pltpu.make_async_copy(wag, grow(core)(0), osem.at[2]))
    keep[2].start()
    ag_h.middle()
    ag_p[2].middle()
    vec_out[...] = shared(vecz, zc, ids_z)
    ag_h.end()
    ag_w.middle()
    ag_p[3].middle()
    ag_w.end()

    ag_h.close()
    ag_w.close()
    for g in ag_p:
        g.end()
    for cp in keep:
        cp.wait()
    for i, cp in enumerate(listed):
        if i != to_sib:
            cp.wait_send()


def train(d, t, h, z, meta, e, w_t, bt, gm, be):
    any_ = pl.BlockSpec(memory_space=pl.ANY)
    vm = pl.BlockSpec(memory_space=pltpu.VMEM)
    sd = jax.ShapeDtypeStruct
    D, BLK, CH, TT, NR, WR = d.D, d.BLK, d.CH, d.TT, d.NR, d.WR

    def vf(*shape):
        return pltpu.VMEM((*shape, D), F32)

    def vl(*shape):
        return pltpu.VMEM(shape, F32)

    def vh(*shape):
        return pltpu.VMEM(shape, BF16)

    def twice(v):
        return [v, v]

    dma = pltpu.SemaphoreType.DMA
    return pl.pallas_call(
        functools.partial(train_kernel, d),
        out_shape=(sd((d.VP, D), F32), sd((d.N, D), F32), sd((D, D), F32), sd((GB, D), F32), sd((2 * NCH, d.CL), F32)),
        in_specs=[any_, any_, any_, vm, any_, vm, vm, vm, vm],
        out_specs=(any_, any_, any_, vm, vm),
        scratch_shapes=[
            vh(d.N, D), vh(2, CH, D), vl(2, NT, CH, TT), vh(2, CH, TT), vf(d.N), vf(16, BLK), *twice(vf(4, BLK)),
            *twice(vf(d.HB)), *twice(vf(BLK)), vf(d.HN), *twice(vf(d.HR)), *twice(vf(NR)),
            vf(NR), *twice(vh(NR, D)), vf(d.HD), *twice(vf(WR // 2)), *twice(vf(WR)), *twice(vf(4, d.WP)), vf(WR),
            vl(8, NT, 8, TT), vl(NT, 8, TT), vl(d.CL, LANES), vl(2 * NCH, d.CL), *twice(vl(4, 2 * NCH, d.CL)),
            *twice(vl(4, GB, LANES)), *twice(vf(GB, GB)), *twice(vf(4, GB)),
            dma((2,)), dma((2,)), dma((2, NT)), dma((3,)), *twice(dma((NSEM,))),
        ],
        compiler_params=pltpu.CompilerParams(vmem_limit_bytes=VMEM_MAX, collective_id=0, has_side_effects=True),
        name="mlm_train",
    )(t, h, z, meta, e, w_t, bt, gm, be)


def finish_kernel(d, cnt_hbm, col_hbm, dh_hbm, de_hbm, dwt_hbm, vec_ref, dbo_ref,
                  dH, dE, dW, g_out, b_out, t_out, loss,
                  cnt, colb, dhb, stage, wstage, outb, isem, csem, osem, dsem, esem, ssem):
    rows_g = GB * d.L
    src_iota = lax.broadcasted_iota(I32, (d.S, rows_g), 1)
    r_iota = lax.broadcasted_iota(I32, (d.S, 1), 0)
    first = pltpu.make_async_copy(cnt_hbm, cnt, ssem.at[0])
    first.start()
    parts = [(c * d.CH, min(d.CH, d.V - c * d.CH)) for c in range(NCH)]
    ins = [pltpu.make_async_copy(de_hbm.at[pl.ds(r, n)], stage.at[pl.ds(r, n)], dsem.at[i])
           for i, (r, n) in enumerate(parts)]
    outs = [pltpu.make_async_copy(stage.at[pl.ds(r, n)], dE.at[pl.ds(r, n)], esem.at[i])
            for i, (r, n) in enumerate(parts)]
    ins.append(pltpu.make_async_copy(dwt_hbm, wstage, dsem.at[NCH]))
    outs.append(pltpu.make_async_copy(wstage, dW, esem.at[NCH]))

    def loads(o, slot):
        o = pl.multiple_of(o, 16)
        return [pltpu.make_async_copy(dh_hbm.at[pl.ds(o, d.S)], dhb.at[slot], isem.at[slot]),
                pltpu.make_async_copy(col_hbm.at[pl.ds(o, d.S)], colb.at[slot], csem.at[slot])]

    def out_copy(g, slot):
        return pltpu.make_async_copy(outb.at[slot], dH.at[pl.ds(g * rows_g, rows_g)], osem.at[slot])

    for cp in loads(jnp.int32(0), 0):
        cp.start()
    for cp in ins:
        cp.start()
    for row, ref in ((LAB, g_out), (LIVE, b_out), (SRC, t_out)):
        for i, cols in enumerate(cuts(d.D)):
            ref[slice(i, i + 1), :] = vec_ref[row, cols]
    loss[...] = dbo_ref[NCH:NCH + 1, LAB]
    first.wait()

    def group(g, o):
        slot = lax.rem(g, 2)
        oslot = lax.rem(g, NBUF)
        c = cnt[0, g * GB]
        for j in range(1, GB):
            c = c + cnt[0, g * GB + j]
        nxt = o + ((c + 15) // 16) * 16

        @pl.when(g + 1 < d.G)
        def _():
            for cp in loads(nxt, 1 - slot):
                cp.start()

        for cp in loads(o, slot):
            cp.wait()

        @pl.when(g >= NBUF)
        def _():
            out_copy(g - NBUF, oslot).wait()

        src = jnp.where(r_iota < c, colb[slot, :, SRC].astype(I32), -1)
        hot = (src_iota == src).astype(BF16)
        outb[oslot] = mm(hot, dhb[slot].astype(BF16), TN).astype(BF16)
        out_copy(g, oslot).start()

        for i, (a, b) in enumerate(zip(ins, outs)):
            @pl.when(g == min(i, d.G - 1))
            def _(a=a, b=b):
                a.wait()
                b.start()

        return nxt

    lax.fori_loop(0, d.G, group, jnp.int32(0))
    for g in range(d.G - NBUF, d.G):
        out_copy(g, g % NBUF).wait()
    for cp in outs:
        cp.wait()


def finish(d, cnt, col, dh, de, dwt, vec, dbo):
    any_ = pl.BlockSpec(memory_space=pl.ANY)
    vm = pl.BlockSpec(memory_space=pltpu.VMEM)
    sd = jax.ShapeDtypeStruct
    dma = pltpu.SemaphoreType.DMA
    row = sd((d.D // LANES, LANES), F32)
    return pl.pallas_call(
        functools.partial(finish_kernel, d),
        out_shape=(sd((d.B * d.L, d.D), BF16), sd((d.V, d.D), F32), sd((d.D, d.D), F32), row, row, row, sd((1, 1), F32)),
        in_specs=[any_, any_, any_, any_, any_, vm, vm],
        out_specs=(any_, any_, any_, vm, vm, vm, vm),
        scratch_shapes=[
            pltpu.SMEM((GB, d.B), I32), pltpu.VMEM((2, d.S, LANES), F32), pltpu.VMEM((2, d.S, d.D), F32),
            pltpu.VMEM((d.VP, d.D), F32), pltpu.VMEM((d.D, d.D), F32), pltpu.VMEM((NBUF, GB * d.L, d.D), BF16),
            dma((2,)), dma((2,)), dma((NBUF,)), dma((NCH + 1,)), dma((NCH + 1,)), dma((1,)),
        ],
        compiler_params=pltpu.CompilerParams(vmem_limit_bytes=VMEM_MAX),
        name="mlm_finish",
    )(cnt, col, dh, de, dwt, vec, dbo)


def solution(mesh):
    def step(hidden, positions, labels, weights, w_t, b_t, gamma, beta, embed, out_bias):
        d = Dims(hidden.shape, positions.shape, embed.shape)
        bias = jnp.pad(out_bias, (0, d.VP - d.V), constant_values=PAD_BIAS).reshape(-1, LANES)
        bt, gm, be = (v.reshape(-1, LANES) for v in (b_t, gamma, beta))
        h, t, z, meta, col, e, cnt = forward(d, hidden.reshape(-1, d.D), positions.T, labels.T, weights.T,
                                             w_t, bt, gm, be, embed, bias)
        de, dh, dwt, vec, dbo = train(d, t, h, z, meta, e, w_t, bt, gm, be)
        d_hidden, d_embed, d_w, d_gamma, d_beta, d_bt, loss = finish(d, cnt, col, dh, de, dwt, vec, dbo)
        d_bias = dbo[:NCH, :d.CH].reshape(-1)[:d.V]
        return (loss.reshape(()), d_hidden.reshape(hidden.shape), d_w, d_bt.reshape(-1), d_gamma.reshape(-1),
                d_beta.reshape(-1), d_embed, d_bias)

    rows, vocab, whole = P("dp"), P("tp"), P()
    return jax.shard_map(step, mesh=mesh, check_vma=False,
                         in_specs=(rows, rows, rows, rows, whole, whole, whole, whole, vocab, vocab),
                         out_specs=(whole, rows, whole, whole, whole, whole, vocab, vocab))
```

```python
import functools

import jax
import jax.numpy as jnp
from jax import lax
from jax.experimental import pallas as pl
from jax.experimental.pallas import tpu as pltpu
from jax.sharding import PartitionSpec as P

F32 = jnp.float32
BF16 = jnp.bfloat16
I32 = jnp.int32
LN_EPS = 1e-12
LOSS_EPS = 1e-5
RSQRT2 = 0.7071067811865476
PAD_BIAS = -3e38
GB = 8
NT = 5
NBUF = 4
VMEM_MAX = 67043328
NCH = 8
NN = (((1,), (0,)), ((), ()))
NTR = (((1,), (1,)), ((), ()))
TN = (((0,), (0,)), ((), ()))


def mm(a, b, dims=NN):
    return lax.dot_general(a, b, dims, preferred_element_type=F32)


LANES = 128
ALL = None
ROWS, COLS = ({"axis": i, "keepdims": True} for i in range(2))
LAB, LIVE, SRC, MAX, SUM, TGT = (slice(i, i + 1) for i in range(6))


class Dims:
    def __init__(self, hidden, positions, embed):
        self.B, self.L, self.D = hidden
        self.P = positions[1]
        self.V = embed[0]
        self.G = self.B // GB
        self.S = GB * self.P
        self.N = self.B * self.P
        self.TT = self.N // NT
        self.BLK = -(-self.V // LANES) * GB
        self.VP = 16 * self.BLK
        self.CH = 2 * self.BLK
        self.NR = self.N // 8
        self.HN, self.HD, self.HB, self.HR = self.N // 2, self.D // 2, self.BLK // 2, self.NR // 2
        self.WR = self.D // 8
        self.WP = self.WR // 4
        self.CL = -(-self.BLK // LANES) * LANES


def cuts(n):
    return [slice(i, min(i + LANES, n)) for i in range(0, n, LANES)]


def row_of(ref):
    return jnp.concatenate([ref[slice(i, i + 1), :] for i in range(ref.shape[0])], axis=1)


def forward_kernel(d, h_hbm, idx_ref, lab_ref, w_ref, wt_ref, bt_ref, gm_ref, be_ref, e_hbm, bias_ref,
                   h_out, t_out, z_out, meta_out, col_out, e_out, cnt_out,
                   hin, hb, tb, ub, eb, bcol, zb, col, meta, keys, cntv, cnt, par3, hsem, esem, zsem, osem):
    rows_g = GB * d.L
    tail = d.V - (NCH - 1) * d.CH

    def h_copy(g, slot):
        return pltpu.make_async_copy(h_hbm.at[pl.ds(g * rows_g, rows_g)], hin.at[slot], hsem.at[slot])

    def e_copy(c):
        n = d.CH if c < NCH - 1 else tail
        return pltpu.make_async_copy(e_hbm.at[pl.ds(c * d.CH, n)], eb.at[pl.ds(c * d.CH, n)], esem.at[c])

    for g in range(NBUF):
        h_copy(g, g).start()
    for c in range(NCH):
        e_copy(c).start()

    cntv[...] = jnp.broadcast_to(jnp.sum(w_ref[...], **ROWS), cntv.shape).astype(I32)
    to_smem = pltpu.make_async_copy(cntv, cnt, osem.at[5])
    to_smem.start()
    outs = [pltpu.make_async_copy(a, b, osem.at[i])
            for i, (a, b) in enumerate(((hb, h_out), (col, col_out), (eb, e_out), (tb, t_out), (meta, meta_out)))]
    outs.append(pltpu.make_async_copy(cntv, cnt_out, osem.at[6]))
    outs[5].start()

    key = lab_ref[...] * 2048 + idx_ref[...] + 1
    keys[...] = jnp.concatenate([key, jnp.zeros((LANES - d.P, d.B), I32)], axis=0).T
    for i, ref in enumerate((bt_ref, gm_ref, be_ref)):
        par3[slice(i, i + 1), :] = row_of(ref)
    hb[...] = jnp.zeros_like(hb)
    tb[...] = jnp.zeros_like(tb)
    col[...] = jnp.zeros_like(col)
    if tail < d.CH:
        eb[d.V:, :] = jnp.zeros((d.VP - d.V, d.D), BF16)
    one_row = lax.broadcasted_iota(I32, (8, d.TT), 0) == 4
    for n in range(NT):
        meta[n] = jnp.where(one_row, 1.0, 0.0)
    for i, rows in enumerate(cuts(d.VP)):
        bcol[rows, :] = jnp.broadcast_to(bias_ref[slice(i, i + 1), :], (LANES, LANES)).T
    to_smem.wait()

    lane = lax.broadcasted_iota(I32, (1, LANES), 1)
    r_iota = lax.broadcasted_iota(I32, (d.S, LANES), 0)
    p_iota = lax.broadcasted_iota(I32, (1, LANES), 1)
    src_iota = lax.broadcasted_iota(I32, (d.S, rows_g), 1)

    def group(g, o):
        slot = lax.rem(g, NBUF)
        off = jnp.int32(0)
        key = jnp.zeros((d.S, LANES), I32)
        for j in range(GB):
            b = g * GB + j
            n_j = cnt[0, b]
            rank = jnp.where(p_iota < n_j, p_iota + off, -1)
            key = key + jnp.where(r_iota == rank, keys[pl.ds(b, 1), :] + j * d.L, 0)
            off = off + n_j
        src = jnp.sum((key & 2047).astype(F32), **COLS)
        lab = jnp.sum((key >> 11).astype(F32), **COLS)
        hot = (src_iota == src.astype(I32) - 1).astype(BF16)
        h_copy(g, slot).wait()
        o = pl.multiple_of(o, 16)
        hb[pl.ds(o, d.S), :] = mm(hot, hin[slot]).astype(BF16)
        live = (src > 0).astype(F32)
        col[pl.ds(o, d.S), :] = jnp.where(lane == 0, lab, jnp.where(lane == 1, live, src - 1))

        @pl.when(g + NBUF < d.G)
        def _():
            h_copy(g + NBUF, slot).start()

        return o + ((off + 15) // 16) * 16

    used = lax.fori_loop(0, d.G, group, jnp.int32(0))
    tiles = (used + d.TT - 1) // d.TT
    outs[0].start()
    outs[1].start()
    for c in range(NCH):
        e_copy(c).wait()
    outs[2].start()

    base_v = lax.axis_index("tp") * d.V
    sub = lax.broadcasted_iota(I32, (8, d.TT), 0)
    rb = min(128, d.TT)

    def z_copy(n, c):
        return pltpu.make_async_copy(zb.at[lax.rem(n, 2), c], z_out.at[n, pl.ds(c * d.CH, d.CH)],
                                     zsem.at[lax.rem(n, 2), c])

    def tile(n, carry):
        par = lax.rem(n, 2)
        base = pl.multiple_of(n * d.TT, d.TT)

        @pl.when(n >= 2)
        def _():
            for c in range(NCH):
                z_copy(n, c).wait()

        ub[...] = mm(hb[pl.ds(base, d.TT), :], wt_ref[...]) + par3[LAB, :]

        def norm(i, carry):
            r = pl.multiple_of(i * rb, rb)
            u = ub[pl.ds(r, rb), :]
            a = 0.5 * u * (1.0 + lax.erf(u * RSQRT2))
            ctr = a - jnp.mean(a, **COLS)
            var = jnp.mean(ctr * ctr, **COLS)
            t = ctr * lax.rsqrt(var + LN_EPS) * par3[LIVE, :] + par3[SRC, :]
            tb[pl.ds(base + r, rb), :] = t.astype(BF16)
            return carry

        lax.fori_loop(0, d.TT // rb, norm, 0)
        for cols in cuts(d.TT):
            blk = col[pl.ds(base + cols.start, LANES), :].T
            meta[n, :3, cols] = blk[:3, :]

        t_n = tb[pl.ds(base, d.TT), :]
        lab = meta[n, LAB, :].astype(I32) - base_v
        lab8 = jnp.broadcast_to(jnp.where(lab < d.V, lab, -1), (8, d.TT))
        m8 = jnp.full((8, d.TT), -jnp.inf, F32)
        s8 = jnp.zeros((8, d.TT), F32)
        t8 = jnp.zeros((8, d.TT), F32)
        reps = d.TT // LANES

        def product(c):
            z = mm(eb[c * d.CH:(c + 1) * d.CH, :], t_n, NTR)
            b = bcol[c * d.CH:(c + 1) * d.CH, :]
            z = z + jnp.concatenate([b] * reps, axis=1)
            zb[par, c] = z
            mx = jnp.max(z.reshape(d.CH // 8, 8, d.TT), axis=0)
            return jnp.broadcast_to(jnp.max(mx, **ROWS), (8, d.TT))

        nxt = product(0)
        for c in range(NCH):
            z_copy(n, c).start()
            mx = jnp.maximum(m8, nxt)
            if c + 1 < NCH:
                nxt = product(c + 1)
            s8 = s8 * jnp.exp(m8 - mx)
            m8 = mx
            for i in range(d.CH // 8):
                zz = zb[par, c, i * 8:(i + 1) * 8, :]
                s8 = s8 + jnp.exp(zz - m8)
                t8 = t8 + jnp.where(sub + (c * d.CH + i * 8) == lab8, zz, 0.0)
        meta[n, MAX, :] = m8[LAB, :]
        meta[n, SUM, :] = jnp.sum(s8, **ROWS)
        meta[n, TGT, :] = jnp.sum(t8, **ROWS)
        return carry

    lax.fori_loop(0, tiles, tile, 0)
    outs[3].start()
    outs[4].start()

    def drain(n, carry):
        for c in range(NCH):
            z_copy(n, c).wait()
        return carry

    lax.fori_loop(jnp.maximum(tiles - 2, 0), tiles, drain, 0)
    for cp in outs:
        cp.wait()


def forward(d, h2, idx, lab, w, w_t, bt, gm, be, embed, bias):
    any_ = pl.BlockSpec(memory_space=pl.ANY)
    vm = pl.BlockSpec(memory_space=pltpu.VMEM)
    sd = jax.ShapeDtypeStruct
    dma = pltpu.SemaphoreType.DMA
    return pl.pallas_call(
        functools.partial(forward_kernel, d),
        out_shape=(sd((d.N, d.D), BF16), sd((d.N, d.D), BF16), sd((NT, d.VP, d.TT), F32), sd((NT, 8, d.TT), F32),
                   sd((d.N, LANES), F32), sd((d.VP, d.D), BF16), sd((8, d.B), I32)),
        in_specs=[any_, vm, vm, vm, vm, vm, vm, vm, any_, vm],
        out_specs=(any_,) * 7,
        scratch_shapes=[
            pltpu.VMEM((NBUF, GB * d.L, d.D), BF16),
            pltpu.VMEM((d.N, d.D), BF16),
            pltpu.VMEM((d.N, d.D), BF16),
            pltpu.VMEM((d.TT, d.D), F32),
            pltpu.VMEM((d.VP, d.D), BF16),
            pltpu.VMEM((d.VP, LANES), F32),
            pltpu.VMEM((2, NCH, d.CH, d.TT), F32),
            pltpu.VMEM((d.N, LANES), F32),
            pltpu.VMEM((NT, 8, d.TT), F32),
            pltpu.VMEM((d.B, LANES), I32),
            pltpu.VMEM((8, d.B), I32),
            pltpu.SMEM((8, d.B), I32),
            pltpu.VMEM((8, d.D), F32),
            dma((NBUF,)), dma((NCH,)), dma((2, NCH)), dma((7,)),
        ],
        compiler_params=pltpu.CompilerParams(vmem_limit_bytes=VMEM_MAX),
        name="mlm_forward",
    )(h2, idx, lab, w, w_t, bt, gm, be, embed, bias)


MESH = pl.DeviceIdType.MESH
RING = (1, 2, 3)
NSEM = 128
NEAR = (2, 1, 3, 0)
CODES = "200210201211110300111301100310101311000010001011"
ORDER = [tuple(int(c) for c in CODES[i:i + 3]) for i in range(0, len(CODES), 3)]
STEPS = "pxxxpxxpppbpbxwvpp00wwvvwpvvww11ww22hhw033h1hww23ww"


def train_kernel(d, t_hbm, h_hbm, z_hbm, meta, e_hbm, wt_ref, bt_ref, gm_ref, be_ref,
                 de_out, dh_out, dwt_out, vec_out, dbo_out,
                 tb, eb, zb, dzb, dt, de, fm, fp, r2a, r2b, f2m, f2p, dr, xa, xb, xm, xp,
                 ub, dub, hown, wr, wxa, wxb, wxm, wxp, wq, wp, w1, w2, w3, w4, wag, srecv, comb, dacc, vb, vby, vbz,
                 dnp, dnq, vec, vect, vecp, vecq, v1, v2, v3, v4, lsem, esem, zsem, osem, ss, rs):
    dp = lax.axis_index("dp")
    tp = lax.axis_index("tp")
    zc, yc = dp // 4, lax.rem(dp, 4)
    x, core = tp // 2, lax.rem(tp, 2)
    other = 1 - core
    pm, qm = 1 + 3 * core, 4 - 3 * core
    p = yc + core * (zc - yc)
    q = zc + core * (yc - zc)
    D, BLK, TT, NR = d.D, d.BLK, d.TT, d.NR
    HN, HD, WR, WP = d.HN, d.HD, d.WR, d.WP

    def rem4(v):
        return lax.rem(v + 4, 4)

    def rem8(v):
        return lax.rem(v + 8, 8)

    def at_p(r):
        return {"dp": rem4(p + r) * pm + q * qm}

    def at_q(r):
        return {"dp": p * pm + rem4(q + r) * qm}

    def at_y(r):
        return {"dp": zc * 4 + rem4(yc + r)}

    def at_z(r):
        return {"dp": rem4(zc + r) * 4 + yc}

    def at_x(r):
        return {"tp": rem4(x + r) * 2 + core}

    def at_t(r):
        return {"tp": rem8(tp + r)}

    sib = {"tp": x * 2 + other}

    def al(v, m=8):
        return pl.multiple_of(v, m)

    listed = []

    def link(src, dst, dev):
        i = len(listed)
        listed.append(pltpu.make_async_remote_copy(src_ref=src, dst_ref=dst, send_sem=ss.at[i], recv_sem=rs.at[i],
                                                   device_id=dev, device_id_type=MESH))
        return i

    def send(src, dst, dev):
        i = link(src, dst, dev)
        listed[i].start()
        return i

    def got(dst, i):
        pltpu.make_async_remote_copy(src_ref=dst, dst_ref=dst, send_sem=ss.at[i], recv_sem=rs.at[i],
                                     device_id=sib, device_id_type=MESH).wait_recv()

    def share(buf, own, at):
        return [send(buf.at[own], buf.at[own], at(r)) for r in RING]

    def shared(buf, own, ids):
        for r, i in zip(RING, ids):
            got(buf.at[rem4(own - r)], i)
        return buf[0] + buf[1] + buf[2] + buf[3]

    def half(ref, h):
        n = ref.shape[0] // 2
        return ref.at[pl.ds(h * n, n)]

    def add(dst, srcs):
        nr = dst.shape[0]
        step = max(s for s in (8, 24, 40) if nr % s == 0)

        def body(i, carry):
            rows = pl.ds(al(i * step), step)
            v = dst[rows, :]
            for s in srcs:
                v = v + s[rows, :]
            dst[rows, :] = v
            return carry

        lax.fori_loop(0, nr // step, body, 0)

    def spot(ref, base, n, h=ALL):
        if h is ALL:
            return ref.at[pl.ds(al(base), n)]
        return ref.at[pl.ds(al(base + h * (n // 2)), n // 2)]

    first_of = (jnp.where((q == 1) | (q == 2), 0, 1), jnp.where((q == 1) | (q == 2), 3, 2))

    def block_id(k):
        out = p * 0
        for i, (rel, h, second) in enumerate(ORDER):
            b = 4 * h + 1 - first_of[h] if second else first_of[h]
            out = jnp.where(k == i, rem4(p + rel) * 4 + b, out)
        return out

    def loads(k):
        slot = lax.rem(k, 2)
        r = block_id(k) * BLK
        return [pltpu.make_async_copy(e_hbm.at[pl.ds(al(r, 16), BLK)], eb.at[slot], esem.at[slot])] + [
            pltpu.make_async_copy(z_hbm.at[n, pl.ds(al(r), BLK)], zb.at[slot, n], zsem.at[slot, n]) for n in range(NT)]

    t_load = pltpu.make_async_copy(t_hbm, tb, lsem.at[0])
    h_load = pltpu.make_async_copy(h_hbm.at[pl.ds(al((core * 4 + x) * NR, 16), NR)], hown, lsem.at[1])
    for cp in loads(jnp.int32(0)):
        cp.start()
    t_load.start()
    h_load.start()

    barrier = pltpu.get_barrier_semaphore()
    peers = [f(r) for f in (at_y, at_z) for r in RING] + [at_t(r) for r in range(1, 8)]
    for dev in peers:
        pl.semaphore_signal(barrier, inc=1, device_id=dev, device_id_type=MESH)
    wsum = jnp.zeros((1, 1), F32)
    for n in range(NT):
        wsum = wsum + jnp.sum(meta[n, LIVE, :], **COLS)
    dnp[yc] = jnp.broadcast_to(wsum, dnp.shape[1:])
    srecv[tp] = meta[...]
    pl.semaphore_wait(barrier, len(peers))

    ids_y = share(dnp, yc, at_y)
    ids_t = [send(meta, srecv.at[tp], at_t(r)) for r in range(1, 8)]
    dt[...] = jnp.zeros_like(dt)
    for k in (*range(8), *range(12, 16)):
        de[k] = jnp.zeros((BLK, D), F32)
    vb[...] = jnp.zeros_like(vb)
    dnq[zc] = shared(dnp, yc, ids_y)
    ids_z = share(dnq, zc, at_z)
    for r, i in zip(range(1, 8), ids_t):
        got(srecv.at[rem8(tp - r)], i)
    tiles = []
    for n in range(NT):
        mx = srecv[0, n, MAX, :]
        for k in range(1, 8):
            mx = jnp.maximum(mx, srecv[k, n, MAX, :])
        tot = jnp.zeros((1, TT), F32)
        tgt = jnp.zeros((1, TT), F32)
        for k in range(8):
            tot = tot + srecv[k, n, SUM, :] * jnp.exp(srecv[k, n, MAX, :] - mx)
            tgt = tgt + srecv[k, n, TGT, :]
        lab = meta[n, LAB, :] - (tp * d.V).astype(F32)
        comb[n, LAB, :] = mx
        comb[n, LIVE, :] = 1.0 / tot
        comb[n, MAX, :] = jnp.where(lab < d.V, lab, -1.0)
        tiles.append(jnp.log(tot) + mx - tgt)
    denom = shared(dnq, zc, ids_z)[LAB, LAB] + LOSS_EPS
    ce = jnp.zeros((1, TT), F32)
    for n in range(NT):
        w = meta[n, LIVE, :]
        c = w / denom
        comb[n, LIVE, :] = comb[n, LIVE, :] * c
        comb[n, SRC, :] = c
        ce = ce + w * tiles[n]
    ce = jnp.sum(ce, **COLS) / denom
    t_load.wait()

    sub = lax.broadcasted_iota(I32, (16, TT), 0)
    row16 = lax.broadcasted_iota(I32, (16, LANES), 0)
    dacc[BLK:, :] = jnp.zeros((d.CL - BLK, LANES), F32)

    def grads(slot, n, cid):
        m8 = jnp.broadcast_to(comb[n, LAB, :], (16, TT))
        a8 = jnp.broadcast_to(comb[n, LIVE, :], (16, TT))
        c8 = jnp.broadcast_to(comb[n, SRC, :], (16, TT))
        l8 = jnp.broadcast_to(comb[n, MAX, :].astype(I32) - cid * BLK, (16, TT))
        live = c8 > 0
        for i in range(BLK // 16):
            rows = slice(i * 16, (i + 1) * 16)
            g = jnp.exp(zb[slot, n, rows, :] - m8) * a8
            g = g - jnp.where(sub + i * 16 == l8, c8, 0.0)
            g = jnp.where(live, g, 0.0)
            dzb[n % 2, rows, :] = g.astype(BF16)
            part = sum(g[:, cols] for cols in cuts(TT))
            dacc[rows, :] = part if n == 0 else dacc[rows, :] + part

    stage1 = [link(de.at[k], de.at[k + 8], at_p(3 if k % 2 else 1)) for k in range(4)]
    stage1 += [link(de.at[k], (fp if k % 2 else fm).at[(k - 4) // 2], at_p(3 if k % 2 else 1)) for k in range(4, 12)]
    to_sib = [link(dt.at[pl.ds(al((other * 4 + rem4(x + r)) * NR), NR)], dr.at[rem4(x + r)], sib) for r in NEAR]

    def step(k, carry):
        slot = lax.rem(k, 2)
        for cp in loads(k):
            cp.wait()

        @pl.when(k < 15)
        def _():
            for cp in loads(k + 1):
                cp.start()

        for i in range(4):
            @pl.when(k == i + 8)
            def _(i=i):
                got(de.at[i + 8], stage1[i])
        cid = block_id(k)
        for n in range(NT):
            grads(slot, n, cid)
            de[k] += mm(dzb[n % 2], tb[n * TT:(n + 1) * TT, :])
            dt[n * TT:(n + 1) * TT, :] += mm(dzb[n % 2], eb[slot], TN)
        for cols in cuts(d.CL):
            tot = jnp.broadcast_to(jnp.sum(dacc[cols, :].T, **ROWS), (16, LANES))
            vb[:16, cols] = jnp.where(row16 == cid, tot, vb[:16, cols])
        for i in range(12):
            @pl.when(k == i)
            def _(i=i):
                listed[stage1[i]].start()

        return carry

    lax.fori_loop(0, 16, step, 0)
    for i in to_sib:
        listed[i].start()
    vb[16:, :] = jnp.broadcast_to(ce, (GB, d.CL))
    vby[yc] = vb[...]
    ids_vy = share(vby, yc, at_y)

    flows = {}
    keep = []

    def copy_out(src, dst):
        keep.append(pltpu.make_async_copy(src, dst, osem.at[len(keep)]))
        keep[-1].start()

    def flow_b():
        yield
        vbz[zc] = shared(vby, yc, ids_vy)
        ids = share(vbz, zc, at_z)
        yield
        dbo_out[...] = shared(vbz, zc, ids)

    def orow(rp, rq, h=ALL):
        return spot(de_out, (rem4(p + rp) * 4 + rem4(q + rq)) * BLK, BLK, h)

    def own(r, h=ALL):
        b = rem4(q + r)
        side = b // 2
        head = first_of[0] + side * (first_of[1] - first_of[0])
        blk = de.at[12 + side + jnp.where(b == head, 0, 2)]
        return blk if h is ALL else half(blk, h)

    def scatter_rest(blk, a, b, m, pp, at, ids):
        yield
        got(a, ids[0])
        add(blk(1, 0), [a])
        ids.append(send(blk(1, 0), half(m, 0), at(1)))
        yield
        got(b, ids[1])
        add(blk(3, 1), [b])
        ids.append(send(blk(3, 1), half(pp, 1), at(3)))

    def scatter_end(m, pp, ids):
        got(half(m, 1), ids[2])
        got(half(pp, 0), ids[3])
        got(half(m, 0), ids[4])
        got(half(pp, 1), ids[5])

    def far(blk, a, b, at):
        return [send(blk(2, 0), a, at(1)), send(blk(2, 1), b, at(3))]

    def near(blk, m, pp, at):
        return [send(blk(1, 1), half(m, 1), at(1)), send(blk(3, 0), half(pp, 0), at(3))]

    def both(src, dst, at):
        return [send(src, dst, at(1)), send(src, dst, at(3))]

    def relay(j):
        ids = both(orow(0, j) if j else own(0), orow(0, j), at_p)
        for r, h in ((3, 0), (1, 1)):
            yield
            got(orow(r, j), ids[h])
            ids.append(send(orow(r, j, h), orow(r, j, h), at_p(1 + 2 * h)))
        yield
        for h in (0, 1):
            got(orow(2, j, h), ids[2 + h])

    def begin(name, gen):
        flows[name] = gen
        return next(gen)

    def flow_p():
        yield
        for k, i in ((4, 13), (5, 12), (6, 15), (7, 14)):
            buf = (fp if k % 2 else fm).at[(k - 4) // 2]
            got(buf, stage1[k])
            add(de.at[i], [buf])
        yield
        for k in (8, 9):
            buf = (fp if k % 2 else fm).at[2]
            got(buf, stage1[k])
            add(de.at[k + 4], [buf])
        ids = far(own, r2a, r2b, at_q)
        yield
        for k in (10, 11):
            buf = (fp if k % 2 else fm).at[3]
            got(buf, stage1[k])
            add(de.at[k + 4], [buf])
        ids += near(own, f2m, f2p, at_q)
        yield from scatter_rest(own, r2a, r2b, f2m, f2p, at_q, ids)
        yield
        scatter_end(f2m, f2p, ids)
        fin = own(0)
        add(fin, [f2m, f2p])
        ids = both(fin, orow(0, 0), at_q)
        copy_out(fin, orow(0, 0))
        begin("0", relay(0))
        for r, h in ((3, 0), (1, 1)):
            yield
            got(orow(0, r), ids[h])
            ids.append(send(orow(0, r, h), orow(0, r, h), at_q(1 + 2 * h)))
            begin("12"[h], relay(r))
        yield
        for h in (0, 1):
            got(orow(0, 2, h), ids[2 + h])
        begin("3", relay(2))

    def xrow(r, h=ALL):
        return spot(dt, (core * 4 + rem4(x + r)) * NR, NR, h)

    def rows_out(out, n):
        def at(c):
            return lambda r, h=ALL: spot(out, (c * 4 + rem4(x + r)) * n, n, h)

        return at(core), at(other)

    def gather_x(src, out, n):
        mine, its = rows_out(out, n)
        ids = both(src, mine(0), at_x)
        sibs = [send(src, mine(0), sib)]
        copy_out(src, mine(0))
        for r, h in ((3, 0), (1, 1)):
            yield
            got(mine(r), ids[h])
            ids.append(send(mine(r, h), mine(r, h), at_x(1 + 2 * h)))
            sibs.append(send(mine(r), mine(r), sib))
        yield
        for h in (0, 1):
            got(mine(2, h), ids[2 + h])
        sibs.append(send(mine(2), mine(2), sib))
        yield
        for r, i in zip((0, 3, 1, 2), sibs):
            got(its(r), i)

    def flow_x():
        def take(*ks):
            for k in ks:
                r = NEAR[k]
                got(dr.at[rem4(x + r)], to_sib[k])
                add(xrow(r), [dr.at[rem4(x + r)]])

        yield
        take(0)
        ids = far(xrow, xa, xb, at_x)
        yield
        take(1, 2)
        ids += near(xrow, xm, xp, at_x)
        yield
        take(3)
        h_load.wait()
        ub[...] = mm(hown[...], wt_ref[...]) + row_of(bt_ref)
        yield from scatter_rest(xrow, xa, xb, xm, xp, at_x, ids)
        yield
        scatter_end(xm, xp, ids)
        layer_back()
        for i in to_sib:
            listed[i].wait_send()
        dwt = dt.at[pl.ds(al(other * HN), D)]
        for cols in cuts(D):
            dwt[:, cols] = mm(hown[...], dub[:, cols], TN)
        i_wr = send(dwt.at[pl.ds(al(other * HD), HD)], wr, sib)
        vect[tp] = jnp.concatenate([jnp.sum(vec[i], **ROWS) for i in range(GB)], axis=0)
        ids = [send(vect.at[tp], vect.at[tp], at_t(r)) for r in range(1, 8)]
        begin("w", flow_w(dwt, i_wr))
        begin("v", flow_v(ids))
        for cols in cuts(D):
            ub[:, cols] = mm(dub[...], wt_ref[cols, :], NTR).astype(BF16).astype(F32)

    lb = 64 if NR % 64 == 0 else 16

    def layer_back():
        dtown = xrow(0)
        gamma = row_of(gm_ref)
        vec[...] = jnp.zeros_like(vec)

        def back(i, carry):
            rows = pl.ds(al(i * lb, 16), lb)
            u = ub[rows, :]
            cdf = 0.5 * (1.0 + lax.erf(u * RSQRT2))
            a = u * cdf
            ctr = a - jnp.mean(a, **COLS)
            rstd = lax.rsqrt(jnp.mean(ctr * ctr, **COLS) + LN_EPS)
            xh = ctr * rstd
            g = dtown[rows, :] + xm[rows, :] + xp[rows, :]
            gx = g * xh
            gg = g * gamma
            m1 = jnp.mean(gg, **COLS)
            m2 = jnp.mean(gg * xh, **COLS)
            da = rstd * (gg - m1 - xh * m2)
            pdf = jnp.exp(u * u * -0.5) * 0.3989422804014327
            du = da * (cdf + u * pdf)
            dub[rows, :] = du.astype(BF16)
            for j, v in enumerate((gx, g, du)):
                vec[j] += jnp.sum(v.reshape(lb // GB, GB, D), axis=0)
            return carry

        lax.fori_loop(0, NR // lb, back, 0)

    def swapped(src, dst, value):
        src[...] = value
        return send(src, dst, sib)

    def flow_w(dwt, i_wr):
        def wrow(r, h=ALL):
            return spot(dwt, core * HD + rem4(x + r) * WR, WR, h)

        def piece(ref, k):
            return ref.at[pl.ds(al(k * WP), WP)]

        yield
        got(wr, i_wr)
        add(dwt.at[pl.ds(al(core * HD), HD)], [wr])
        ids = far(wrow, wxa, wxb, at_x) + near(wrow, wxm, wxp, at_x)
        yield from scatter_rest(wrow, wxa, wxb, wxm, wxp, at_x, ids)
        begin("h", gather_x(ub, dh_out, NR))
        yield
        scatter_end(wxm, wxp, ids)
        mine = wrow(0)
        add(mine, [wxm, wxp])
        ids = [send(piece(mine, rem4(q + r)), wq.at[q], at_q(r)) for r in RING]
        wq[q] = piece(mine, q)[...]
        yield
        i = swapped(w1, w2, shared(wq, q, ids))
        yield
        got(w2, i)
        wp[q] = w2[...]
        ids = share(wp, q, at_q)
        yield
        i = swapped(w3, w4, shared(wp, q, ids))
        yield
        got(w4, i)
        piece(wag, q)[...] = w4[...]
        ids = [send(piece(wag, q), piece(wag, q), at_q(r)) for r in RING]
        yield
        for r, i in zip(RING, ids):
            got(piece(wag, rem4(q - r)), i)
        yield from gather_x(wag, dwt_out, WR)

    def flow_v(ids):
        yield
        for r, i in zip(range(1, 8), ids):
            got(vect.at[rem8(tp - r)], i)
        vecq[q] = sum(vect[k] for k in range(8))
        ids = share(vecq, q, at_q)
        yield
        i = swapped(v1, v2, shared(vecq, q, ids))
        yield
        got(v2, i)
        vecp[q] = v2[...]
        ids = share(vecp, q, at_q)
        yield
        total = shared(vecp, q, ids)
        i = swapped(v3, v4, total)
        yield
        got(v4, i)
        vec_out[...] = jnp.where(core == 0, v3[...], v4[...])

    for name, gen in (("p", flow_p()), ("x", flow_x()), ("b", flow_b())):
        begin(name, gen)
    for name in STEPS:
        next(flows[name], 0)
    for gen in flows.values():
        assert next(gen, ALL) is ALL and gen.gi_frame is ALL

    for cp in keep:
        cp.wait()
    for i, cp in enumerate(listed):
        if i not in to_sib:
            cp.wait_send()


def train(d, t, h, z, meta, e, w_t, bt, gm, be):
    any_ = pl.BlockSpec(memory_space=pl.ANY)
    vm = pl.BlockSpec(memory_space=pltpu.VMEM)
    sd = jax.ShapeDtypeStruct
    D, BLK, TT, NR, WR = d.D, d.BLK, d.TT, d.NR, d.WR

    def vf(*shape):
        return pltpu.VMEM((*shape, D), F32)

    def vl(*shape):
        return pltpu.VMEM(shape, F32)

    def vh(*shape):
        return pltpu.VMEM(shape, BF16)

    def twice(v):
        return [v, v]

    dma = pltpu.SemaphoreType.DMA
    return pl.pallas_call(
        functools.partial(train_kernel, d),
        out_shape=(sd((d.VP, D), F32), sd((d.N, D), F32), sd((D, D), F32), sd((GB, D), F32), sd((3 * GB, d.CL), F32)),
        in_specs=[any_, any_, any_, vm, any_, vm, vm, vm, vm],
        out_specs=(any_, any_, any_, vm, vm),
        scratch_shapes=[
            vh(d.N, D), vh(2, BLK, D), vl(2, NT, BLK, TT), vh(2, BLK, TT), vf(d.N), vf(16, BLK), *twice(vf(4, BLK)),
            *twice(vf(d.HB)), *twice(vf(BLK)), vf(4, NR), *twice(vf(d.HR)), *twice(vf(NR)),
            vf(NR), *twice(vh(NR, D)), vf(d.HD), *twice(vf(WR // 2)), *twice(vf(WR)), *twice(vf(4, d.WP)), *twice(vf(d.WP)), *twice(vf(d.WP)), vf(WR),
            vl(8, NT, 8, TT), vl(NT, 8, TT), vl(d.CL, LANES), vl(3 * GB, d.CL), *twice(vl(4, 3 * GB, d.CL)),
            *twice(vl(4, GB, LANES)), *twice(vf(GB, GB)), *twice(vf(4, GB)), *twice(vf(GB)), *twice(vf(GB)),
            dma((2,)), dma((2,)), dma((2, NT)), dma((3,)), *twice(dma((NSEM,))),
        ],
        compiler_params=pltpu.CompilerParams(vmem_limit_bytes=VMEM_MAX, collective_id=0, has_side_effects=True),
        name="mlm_train",
    )(t, h, z, meta, e, w_t, bt, gm, be)


def finish_kernel(d, cnt_hbm, col_hbm, dh_hbm, de_hbm, dwt_hbm, vec_ref, dbo_ref,
                  dH, dE, dW, g_out, b_out, t_out, loss,
                  cnt, colb, dhb, stage, wstage, outb, isem, csem, osem, dsem, esem, ssem):
    rows_g = GB * d.L
    src_iota = lax.broadcasted_iota(I32, (d.S, rows_g), 1)
    r_iota = lax.broadcasted_iota(I32, (d.S, 1), 0)
    first = pltpu.make_async_copy(cnt_hbm, cnt, ssem.at[0])
    first.start()
    parts = [(c * d.CH, min(d.CH, d.V - c * d.CH)) for c in range(NCH)]
    ins = [pltpu.make_async_copy(de_hbm.at[pl.ds(r, n)], stage.at[pl.ds(r, n)], dsem.at[i])
           for i, (r, n) in enumerate(parts)]
    outs = [pltpu.make_async_copy(stage.at[pl.ds(r, n)], dE.at[pl.ds(r, n)], esem.at[i])
            for i, (r, n) in enumerate(parts)]
    ins.append(pltpu.make_async_copy(dwt_hbm, wstage, dsem.at[NCH]))
    outs.append(pltpu.make_async_copy(wstage, dW, esem.at[NCH]))

    def loads(o, slot):
        o = pl.multiple_of(o, 16)
        return [pltpu.make_async_copy(dh_hbm.at[pl.ds(o, d.S)], dhb.at[slot], isem.at[slot]),
                pltpu.make_async_copy(col_hbm.at[pl.ds(o, d.S)], colb.at[slot], csem.at[slot])]

    def out_copy(g, slot):
        return pltpu.make_async_copy(outb.at[slot], dH.at[pl.ds(g * rows_g, rows_g)], osem.at[slot])

    for cp in loads(jnp.int32(0), 0):
        cp.start()
    for cp in ins:
        cp.start()
    for row, ref in ((LAB, g_out), (LIVE, b_out), (SRC, t_out)):
        for i, cols in enumerate(cuts(d.D)):
            ref[slice(i, i + 1), :] = vec_ref[row, cols]
    loss[...] = dbo_ref[16:17, LAB]
    first.wait()

    def group(g, o):
        slot = lax.rem(g, 2)
        oslot = lax.rem(g, NBUF)
        c = cnt[0, g * GB]
        for j in range(1, GB):
            c = c + cnt[0, g * GB + j]
        nxt = o + ((c + 15) // 16) * 16

        @pl.when(g + 1 < d.G)
        def _():
            for cp in loads(nxt, 1 - slot):
                cp.start()

        for cp in loads(o, slot):
            cp.wait()

        @pl.when(g >= NBUF)
        def _():
            out_copy(g - NBUF, oslot).wait()

        src = jnp.where(r_iota < c, colb[slot, :, SRC].astype(I32), -1)
        hot = (src_iota == src).astype(BF16)
        outb[oslot] = mm(hot, dhb[slot].astype(BF16), TN).astype(BF16)
        out_copy(g, oslot).start()

        for i, (a, b) in enumerate(zip(ins, outs)):
            @pl.when(g == min(i, d.G - 1))
            def _(a=a, b=b):
                a.wait()
                b.start()

        return nxt

    lax.fori_loop(0, d.G, group, jnp.int32(0))
    for g in range(d.G - NBUF, d.G):
        out_copy(g, g % NBUF).wait()
    for cp in outs:
        cp.wait()


def finish(d, cnt, col, dh, de, dwt, vec, dbo):
    any_ = pl.BlockSpec(memory_space=pl.ANY)
    vm = pl.BlockSpec(memory_space=pltpu.VMEM)
    sd = jax.ShapeDtypeStruct
    dma = pltpu.SemaphoreType.DMA
    row = sd((d.D // LANES, LANES), F32)
    return pl.pallas_call(
        functools.partial(finish_kernel, d),
        out_shape=(sd((d.B * d.L, d.D), BF16), sd((d.V, d.D), F32), sd((d.D, d.D), F32), row, row, row, sd((1, 1), F32)),
        in_specs=[any_, any_, any_, any_, any_, vm, vm],
        out_specs=(any_, any_, any_, vm, vm, vm, vm),
        scratch_shapes=[
            pltpu.SMEM((GB, d.B), I32), pltpu.VMEM((2, d.S, LANES), F32), pltpu.VMEM((2, d.S, d.D), F32),
            pltpu.VMEM((d.VP, d.D), F32), pltpu.VMEM((d.D, d.D), F32), pltpu.VMEM((NBUF, GB * d.L, d.D), BF16),
            dma((2,)), dma((2,)), dma((NBUF,)), dma((NCH + 1,)), dma((NCH + 1,)), dma((1,)),
        ],
        compiler_params=pltpu.CompilerParams(vmem_limit_bytes=VMEM_MAX),
        name="mlm_finish",
    )(cnt, col, dh, de, dwt, vec, dbo)


def solution(mesh):
    def step(hidden, positions, labels, weights, w_t, b_t, gamma, beta, embed, out_bias):
        d = Dims(hidden.shape, positions.shape, embed.shape)
        bias = jnp.pad(out_bias, (0, d.VP - d.V), constant_values=PAD_BIAS).reshape(-1, LANES)
        bt, gm, be = (v.reshape(-1, LANES) for v in (b_t, gamma, beta))
        h, t, z, meta, col, e, cnt = forward(d, hidden.reshape(-1, d.D), positions.T, labels.T, weights.T,
                                             w_t, bt, gm, be, embed, bias)
        de, dh, dwt, vec, dbo = train(d, t, h, z, meta, e, w_t, bt, gm, be)
        d_hidden, d_embed, d_w, d_gamma, d_beta, d_bt, loss = finish(d, cnt, col, dh, de, dwt, vec, dbo)
        d_bias = dbo[:16, :d.BLK].reshape(-1)[:d.V]
        return (loss.reshape(()), d_hidden.reshape(hidden.shape), d_w, d_bt.reshape(-1), d_gamma.reshape(-1),
                d_beta.reshape(-1), d_embed, d_bias)

    rows, vocab, whole = P("dp"), P("tp"), P()
    return jax.shard_map(step, mesh=mesh, check_vma=False,
                         in_specs=(rows, rows, rows, rows, whole, whole, whole, whole, vocab, vocab),
                         out_specs=(whole, rows, whole, whole, whole, whole, vocab, vocab))
```

```python
import functools

import jax
import jax.numpy as jnp
from jax import lax
from jax.experimental import pallas as pl
from jax.experimental.pallas import tpu as pltpu
from jax.sharding import PartitionSpec as P

F32 = jnp.float32
BF16 = jnp.bfloat16
I32 = jnp.int32
LN_EPS = 1e-12
LOSS_EPS = 1e-5
RSQRT2 = 0.7071067811865476
PAD_BIAS = -3e38
GB = 8
NT = 5
NBUF = 4
VMEM_MAX = 67043328
NCH = 8
NN = (((1,), (0,)), ((), ()))
NTR = (((1,), (1,)), ((), ()))
TN = (((0,), (0,)), ((), ()))


def mm(a, b, dims=NN):
    return lax.dot_general(a, b, dims, preferred_element_type=F32)


LANES = 128
ALL = None
ROWS, COLS = ({"axis": i, "keepdims": True} for i in range(2))
LAB, LIVE, SRC, MAX, SUM, TGT = (slice(i, i + 1) for i in range(6))


class Dims:
    def __init__(self, hidden, positions, embed):
        self.B, self.L, self.D = hidden
        self.P = positions[1]
        self.V = embed[0]
        self.G = self.B // GB
        self.S = GB * self.P
        self.N = self.B * self.P
        self.TT = self.N // NT
        self.BLK = -(-self.V // LANES) * GB
        self.VP = 16 * self.BLK
        self.CH = 2 * self.BLK
        self.NR = self.N // 8
        self.HN, self.HD, self.HB, self.HR = self.N // 2, self.D // 2, self.BLK // 2, self.NR // 2
        self.WR = self.D // 8
        self.WP = self.WR // 4
        self.CL = -(-self.BLK // LANES) * LANES


def cuts(n):
    return [slice(i, min(i + LANES, n)) for i in range(0, n, LANES)]


def row_of(ref):
    return jnp.concatenate([ref[slice(i, i + 1), :] for i in range(ref.shape[0])], axis=1)


def forward_kernel(d, h_hbm, idx_ref, lab_ref, w_ref, wt_ref, bt_ref, gm_ref, be_ref, e_hbm, bias_ref,
                   h_out, t_out, z_out, meta_out, col_out, e_out, cnt_out,
                   hin, hb, tb, ub, eb, bcol, zb, col, meta, keys, cntv, cnt, par3, hot_a, hot_b, zero, hsem, esem, zsem, tsem, fsem, osem):
    rows_g = GB * d.L
    tail = d.V - (NCH - 1) * d.CH

    def h_copy(g, slot):
        return pltpu.make_async_copy(h_hbm.at[pl.ds(g * rows_g, rows_g)], hin.at[slot], hsem.at[slot])

    def e_copy(c):
        n = d.CH if c < NCH - 1 else tail
        return pltpu.make_async_copy(e_hbm.at[pl.ds(c * d.CH, n)], eb.at[pl.ds(c * d.CH, n)], esem.at[c])

    for g in range(NBUF):
        h_copy(g, g).start()
    for c in range(NCH):
        e_copy(c).start()

    cntv[...] = jnp.broadcast_to(jnp.sum(w_ref[...], **ROWS), cntv.shape).astype(I32)
    to_smem = pltpu.make_async_copy(cntv, cnt, osem.at[5])
    to_smem.start()
    outs = [pltpu.make_async_copy(a, b, osem.at[i])
            for i, (a, b) in enumerate(((hb, h_out), (col, col_out), (eb, e_out), (meta, meta_out)))]
    outs.append(pltpu.make_async_copy(cntv, cnt_out, osem.at[6]))
    outs[4].start()

    key = lab_ref[...] * 2048 + idx_ref[...] + 1
    keys[...] = jnp.concatenate([key, jnp.zeros((LANES - d.P, d.B), I32)], axis=0).T
    for i, ref in enumerate((bt_ref, gm_ref, be_ref)):
        par3[slice(i, i + 1), :] = row_of(ref)
    hb[...] = jnp.zeros_like(hb)
    tb[...] = jnp.zeros_like(tb)
    col[...] = jnp.zeros_like(col)
    if tail < d.CH:
        eb[d.V:, :] = jnp.zeros((d.VP - d.V, d.D), BF16)
    one_row = lax.broadcasted_iota(I32, (8, d.TT), 0) == 4
    for n in range(NT):
        meta[n] = jnp.where(one_row, 1.0, 0.0)
    for i, rows in enumerate(cuts(d.VP)):
        bcol[rows, :] = jnp.broadcast_to(bias_ref[slice(i, i + 1), :], (LANES, LANES)).T
    to_smem.wait()

    lane = lax.broadcasted_iota(I32, (1, LANES), 1)
    r_iota = lax.broadcasted_iota(I32, (d.S, LANES), 0)
    p_iota = lax.broadcasted_iota(I32, (1, LANES), 1)
    src_iota = lax.broadcasted_iota(I32, (d.S, rows_g), 1)

    def pick(g, hot):
        off = jnp.int32(0)
        key = jnp.zeros((d.S, LANES), I32)
        for j in range(GB):
            b = g * GB + j
            n_j = cnt[0, b]
            rank = jnp.where(p_iota < n_j, p_iota + off, -1)
            key = key + jnp.where(r_iota == rank, keys[pl.ds(b, 1), :] + j * d.L, 0)
            off = off + n_j
        src = jnp.sum((key & 2047).astype(F32), **COLS)
        lab = jnp.sum((key >> 11).astype(F32), **COLS)
        hot[...] = (src_iota == src.astype(I32) - 1).astype(BF16)
        live = (src > 0).astype(F32)
        return off, jnp.where(lane == 0, lab, jnp.where(lane == 1, live, src - 1))

    def pair(i, carry):
        o, n, cols = carry
        for k, (hot, nxt) in enumerate(((hot_a, hot_b), (hot_b, hot_a))):
            g = 2 * i + k
            slot = lax.rem(g, NBUF)
            h_copy(g, slot).wait()
            o = pl.multiple_of(o, 16)
            hb[pl.ds(o, d.S), :] = mm(hot[...], hin[slot]).astype(BF16)
            col[pl.ds(o, d.S), :] = cols
            o = o + ((n + 15) // 16) * 16
            n, cols = pick(jnp.minimum(g + 1, d.G - 1), nxt)

            @pl.when(g + NBUF < d.G)
            def _():
                h_copy(g + NBUF, slot).start()

        return o, n, cols

    used, _, _ = lax.fori_loop(0, d.G // 2, pair, (jnp.int32(0), *pick(0, hot_a)))
    tiles = (used + d.TT - 1) // d.TT
    outs[0].start()
    outs[1].start()
    for c in range(NCH):
        e_copy(c).wait()
    outs[2].start()

    base_v = lax.axis_index("tp") * d.V
    sub = lax.broadcasted_iota(I32, (GB, LANES), 0)
    rb = min(LANES, d.TT)
    reps = d.TT // LANES

    def z_copy(n, c):
        par = lax.rem(n, 2)
        return pltpu.make_async_copy(zb.at[par, c], z_out.at[n, pl.ds(c * d.CH, d.CH)], zsem.at[par, c])

    def z_fill(n, c):
        return pltpu.make_async_copy(zero, z_out.at[n, pl.ds(c * d.CH, d.CH)], fsem.at[n, c])

    def fill(n, carry):
        for c in range(NCH):
            z_fill(n, c).start()
        return carry

    zero[...] = jnp.zeros_like(zero)
    lax.fori_loop(tiles, NT, fill, 0)

    def t_copy(n):
        rows = pl.ds(pl.multiple_of(n * d.TT, d.TT), d.TT)
        return pltpu.make_async_copy(tb.at[rows], t_out.at[rows], tsem.at[n])

    def dense(n):
        ub[...] = mm(hb[pl.ds(pl.multiple_of(n * d.TT, d.TT), d.TT), :], wt_ref[...]) + par3[LAB, :]

    def norm(n, i):
        u = ub[i * rb:(i + 1) * rb, :]
        a = 0.5 * u * (1 + lax.erf(u * RSQRT2))
        ctr = a - jnp.mean(a, **COLS)
        var = jnp.mean(ctr * ctr, **COLS)
        t = ctr * lax.rsqrt(var + LN_EPS) * par3[LIVE, :] + par3[SRC, :]
        tb[pl.ds(pl.multiple_of(n * d.TT + i * rb, rb), rb), :] = t.astype(BF16)

    def wide(v):
        return jnp.concatenate([v] * reps, axis=1)

    def product(n, c):
        rows = slice(c * d.CH, (c + 1) * d.CH)
        t_n = tb[pl.ds(pl.multiple_of(n * d.TT, d.TT), d.TT), :]
        z = mm(eb[rows, :], t_n, NTR) + wide(bcol[rows, :])
        zb[lax.rem(n, 2), c] = z
        mx = jnp.max(z.reshape(d.CH // GB, GB, d.TT), axis=0)
        return jnp.broadcast_to(jnp.max(mx, **ROWS), (GB, d.TT))

    def tile(n, carry):
        par = lax.rem(n, 2)
        base = pl.multiple_of(n * d.TT, d.TT)
        after = jnp.minimum(n + 1, NT - 1)
        t_copy(n).start()

        @pl.when(n >= 2)
        def _():
            for c in range(NCH):
                z_copy(n, c).wait()

        for cols in cuts(d.TT):
            blk = col[pl.ds(base + cols.start, LANES), :].T
            meta[n, :3, cols] = blk[:3, :]
        lab = meta[n, LAB, :].astype(I32) - base_v
        lab8 = jnp.broadcast_to(jnp.where(lab < d.V, lab, -1), (GB, d.TT))
        m8 = jnp.full((GB, d.TT), -jnp.inf, F32)
        s8 = jnp.zeros((GB, d.TT), F32)
        t8 = jnp.zeros((GB, d.TT), F32)
        nxt = product(n, 0)
        dense(after)
        for c in range(NCH):
            z_copy(n, c).start()
            mx = jnp.maximum(m8, nxt)
            if c + 1 < NCH:
                nxt = product(n, c + 1)
            s8 = s8 * jnp.exp(m8 - mx)
            m8 = mx
            zz = zb[par, c].reshape(d.CH // GB, GB, d.TT)
            s8 = s8 + jnp.sum(jnp.exp(zz - m8[None]), axis=0)
            at = lax.broadcasted_iota(I32, zz.shape, 0) * GB + lax.broadcasted_iota(I32, zz.shape, 1) + c * d.CH
            t8 = t8 + jnp.sum(jnp.where(at == lab8[None], zz, 0.0), axis=0)
            if c >= 4 and c - 4 < d.TT // rb:
                norm(after, c - 4)
        meta[n, MAX, :] = m8[LAB, :]
        meta[n, SUM, :] = jnp.sum(s8, **ROWS)
        meta[n, TGT, :] = jnp.sum(t8, **ROWS)
        return carry

    dense(0)
    for i in range(d.TT // rb):
        norm(0, i)
    lax.fori_loop(0, tiles, tile, 0)
    outs[3].start()

    def rest(n, carry):
        t_copy(n).start()
        return carry

    lax.fori_loop(tiles, NT, rest, 0)
    def drain(n, carry):
        for c in range(NCH):
            z_copy(n, c).wait()
        return carry

    lax.fori_loop(jnp.maximum(tiles - 2, 0), tiles, drain, 0)

    def filled(n, carry):
        for c in range(NCH):
            z_fill(n, c).wait()
        return carry

    lax.fori_loop(tiles, NT, filled, 0)
    for n in range(NT):
        t_copy(n).wait()
    for cp in outs:
        cp.wait()


def forward(d, h2, idx, lab, w, w_t, bt, gm, be, embed, bias):
    any_ = pl.BlockSpec(memory_space=pl.ANY)
    vm = pl.BlockSpec(memory_space=pltpu.VMEM)
    sd = jax.ShapeDtypeStruct
    dma = pltpu.SemaphoreType.DMA
    return pl.pallas_call(
        functools.partial(forward_kernel, d),
        out_shape=(sd((d.N, d.D), BF16), sd((d.N, d.D), BF16), sd((NT, d.VP, d.TT), F32), sd((NT, 8, d.TT), F32),
                   sd((d.N, LANES), F32), sd((d.VP, d.D), BF16), sd((8, d.B), I32)),
        in_specs=[any_, vm, vm, vm, vm, vm, vm, vm, any_, vm],
        out_specs=(any_,) * 7,
        scratch_shapes=[
            pltpu.VMEM((NBUF, GB * d.L, d.D), BF16),
            pltpu.VMEM((d.N, d.D), BF16),
            pltpu.VMEM((d.N, d.D), BF16),
            pltpu.VMEM((d.TT, d.D), F32),
            pltpu.VMEM((d.VP, d.D), BF16),
            pltpu.VMEM((d.VP, LANES), F32),
            pltpu.VMEM((2, NCH, d.CH, d.TT), F32),
            pltpu.VMEM((d.N, LANES), F32),
            pltpu.VMEM((NT, 8, d.TT), F32),
            pltpu.VMEM((d.B, LANES), I32),
            pltpu.VMEM((8, d.B), I32),
            pltpu.SMEM((8, d.B), I32),
            pltpu.VMEM((8, d.D), F32),
            pltpu.VMEM((d.S, GB * d.L), BF16),
            pltpu.VMEM((d.S, GB * d.L), BF16),
            pltpu.VMEM((d.CH, d.TT), F32),
            dma((NBUF,)), dma((NCH,)), dma((2, NCH)), dma((NT,)), dma((NT, NCH)), dma((7,)),
        ],
        compiler_params=pltpu.CompilerParams(vmem_limit_bytes=VMEM_MAX),
        name="mlm_forward",
    )(h2, idx, lab, w, w_t, bt, gm, be, embed, bias)


MESH = pl.DeviceIdType.MESH
RING = (1, 2, 3)
NSEM = 128
NEAR = (2, 1, 3, 0)
CODES = "200210201211110300111301100310101311000010001011"
ORDER = [tuple(int(c) for c in CODES[i:i + 3]) for i in range(0, len(CODES), 3)]
STEPS = "pxxxpxxpppbpbxwvpp00wwvvwpvvww11ww22hhw033h1hww23ww"


def train_kernel(d, t_hbm, h_hbm, z_hbm, meta, e_hbm, wt_ref, bt_ref, gm_ref, be_ref,
                 de_out, dh_out, dwt_out, vec_out, dbo_out,
                 tb, eb, zb, dzb, dt, de, fm, fp, r2a, r2b, f2m, f2p, dr, xa, xb, xm, xp,
                 ub, dub, hown, wr, wxa, wxb, wxm, wxp, wq, wp, w1, w2, w3, w4, wag, srecv, comb, dacc, vb, vby, vbz,
                 dnp, dnq, vec, vect, vecp, vecq, v1, v2, v3, v4, lsem, esem, zsem, osem, ss, rs):
    dp = lax.axis_index("dp")
    tp = lax.axis_index("tp")
    zc, yc = dp // 4, lax.rem(dp, 4)
    x, core = tp // 2, lax.rem(tp, 2)
    other = 1 - core
    pm, qm = 1 + 3 * core, 4 - 3 * core
    p = yc + core * (zc - yc)
    q = zc + core * (yc - zc)
    D, BLK, TT, NR = d.D, d.BLK, d.TT, d.NR
    HN, HD, WR, WP = d.HN, d.HD, d.WR, d.WP

    def rem4(v):
        return lax.rem(v + 4, 4)

    def rem8(v):
        return lax.rem(v + 8, 8)

    def at_p(r):
        return {"dp": rem4(p + r) * pm + q * qm}

    def at_q(r):
        return {"dp": p * pm + rem4(q + r) * qm}

    def at_y(r):
        return {"dp": zc * 4 + rem4(yc + r)}

    def at_z(r):
        return {"dp": rem4(zc + r) * 4 + yc}

    def at_x(r):
        return {"tp": rem4(x + r) * 2 + core}

    def at_t(r):
        return {"tp": rem8(tp + r)}

    sib = {"tp": x * 2 + other}

    def al(v, m=8):
        return pl.multiple_of(v, m)

    listed = []

    def link(src, dst, dev):
        i = len(listed)
        listed.append(pltpu.make_async_remote_copy(src_ref=src, dst_ref=dst, send_sem=ss.at[i], recv_sem=rs.at[i],
                                                   device_id=dev, device_id_type=MESH))
        return i

    def send(src, dst, dev):
        i = link(src, dst, dev)
        listed[i].start()
        return i

    def got(dst, i):
        pltpu.make_async_remote_copy(src_ref=dst, dst_ref=dst, send_sem=ss.at[i], recv_sem=rs.at[i],
                                     device_id=sib, device_id_type=MESH).wait_recv()

    def share(buf, own, at):
        return [send(buf.at[own], buf.at[own], at(r)) for r in RING]

    def shared(buf, own, ids):
        for r, i in zip(RING, ids):
            got(buf.at[rem4(own - r)], i)
        return buf[0] + buf[1] + buf[2] + buf[3]

    def half(ref, h):
        n = ref.shape[0] // 2
        return ref.at[pl.ds(h * n, n)]

    def add(dst, srcs):
        nr = dst.shape[0]
        step = max(s for s in (8, 24, 40) if nr % s == 0)

        def body(i, carry):
            rows = pl.ds(al(i * step), step)
            v = dst[rows, :]
            for s in srcs:
                v = v + s[rows, :]
            dst[rows, :] = v
            return carry

        lax.fori_loop(0, nr // step, body, 0)

    def spot(ref, base, n, h=ALL):
        if h is ALL:
            return ref.at[pl.ds(al(base), n)]
        return ref.at[pl.ds(al(base + h * (n // 2)), n // 2)]

    first_of = (jnp.where((q == 1) | (q == 2), 0, 1), jnp.where((q == 1) | (q == 2), 3, 2))

    def block_id(k):
        out = p * 0
        for i, (rel, h, second) in enumerate(ORDER):
            b = 4 * h + 1 - first_of[h] if second else first_of[h]
            out = jnp.where(k == i, rem4(p + rel) * 4 + b, out)
        return out

    def loads(k):
        slot = lax.rem(k, 2)
        r = block_id(k) * BLK
        return [pltpu.make_async_copy(e_hbm.at[pl.ds(al(r, 16), BLK)], eb.at[slot], esem.at[slot])] + [
            pltpu.make_async_copy(z_hbm.at[n, pl.ds(al(r), BLK)], zb.at[slot, n], zsem.at[slot, n]) for n in range(NT)]

    t_load = pltpu.make_async_copy(t_hbm, tb, lsem.at[0])
    h_load = pltpu.make_async_copy(h_hbm.at[pl.ds(al((core * 4 + x) * NR, 16), NR)], hown, lsem.at[1])
    for cp in loads(jnp.int32(0)):
        cp.start()
    t_load.start()
    h_load.start()

    barrier = pltpu.get_barrier_semaphore()
    peers = [f(r) for f in (at_y, at_z) for r in RING] + [at_t(r) for r in range(1, 8)]
    for dev in peers:
        pl.semaphore_signal(barrier, inc=1, device_id=dev, device_id_type=MESH)
    wsum = jnp.zeros((1, 1), F32)
    for n in range(NT):
        wsum = wsum + jnp.sum(meta[n, LIVE, :], **COLS)
    dnp[yc] = jnp.broadcast_to(wsum, dnp.shape[1:])
    srecv[tp] = meta[...]
    pl.semaphore_wait(barrier, len(peers))

    ids_y = share(dnp, yc, at_y)
    ids_t = [send(meta, srecv.at[tp], at_t(r)) for r in range(1, 8)]
    dt[...] = jnp.zeros_like(dt)
    for k in (*range(8), *range(12, 16)):
        de[k] = jnp.zeros((BLK, D), F32)
    vb[...] = jnp.zeros_like(vb)
    dnq[zc] = shared(dnp, yc, ids_y)
    ids_z = share(dnq, zc, at_z)
    for r, i in zip(range(1, 8), ids_t):
        got(srecv.at[rem8(tp - r)], i)
    tiles = []
    for n in range(NT):
        mx = srecv[0, n, MAX, :]
        for k in range(1, 8):
            mx = jnp.maximum(mx, srecv[k, n, MAX, :])
        tot = jnp.zeros((1, TT), F32)
        tgt = jnp.zeros((1, TT), F32)
        for k in range(8):
            tot = tot + srecv[k, n, SUM, :] * jnp.exp(srecv[k, n, MAX, :] - mx)
            tgt = tgt + srecv[k, n, TGT, :]
        lab = meta[n, LAB, :] - (tp * d.V).astype(F32)
        comb[n, LAB, :] = mx
        comb[n, LIVE, :] = 1.0 / tot
        comb[n, MAX, :] = jnp.where(lab < d.V, lab, -1.0)
        tiles.append(jnp.log(tot) + mx - tgt)
    denom = shared(dnq, zc, ids_z)[LAB, LAB] + LOSS_EPS
    ce = jnp.zeros((1, TT), F32)
    for n in range(NT):
        w = meta[n, LIVE, :]
        c = w / denom
        comb[n, LIVE, :] = comb[n, LIVE, :] * c
        comb[n, SRC, :] = c
        ce = ce + w * tiles[n]
    ce = jnp.sum(ce, **COLS) / denom
    t_load.wait()

    sub = lax.broadcasted_iota(I32, (16, LANES), 0)
    row16 = lax.broadcasted_iota(I32, (16, LANES), 0)
    dacc[BLK:, :] = jnp.zeros((d.CL - BLK, LANES), F32)

    def grads(slot, n, cid):
        m8 = jnp.broadcast_to(comb[n, LAB, :], (16, TT))
        a8 = jnp.broadcast_to(comb[n, LIVE, :], (16, TT))
        c8 = jnp.broadcast_to(comb[n, SRC, :], (16, TT))
        l8 = jnp.broadcast_to(comb[n, MAX, :].astype(I32) - cid * BLK, (16, TT))
        for i in range(BLK // 16):
            rows = slice(i * 16, (i + 1) * 16)
            g = jnp.exp(zb[slot, n, rows, :] - m8) * a8
            at = jnp.concatenate([sub + i * 16] * (TT // LANES), axis=1)
            g = g - jnp.where(at == l8, c8, 0.0)
            dzb[n % 2, rows, :] = g.astype(BF16)
            part = sum(g[:, cols] for cols in cuts(TT))
            dacc[rows, :] = part if n == 0 else dacc[rows, :] + part

    stage1 = [link(de.at[k], de.at[k + 8], at_p(3 if k % 2 else 1)) for k in range(4)]
    stage1 += [link(de.at[k], (fp if k % 2 else fm).at[(k - 4) // 2], at_p(3 if k % 2 else 1)) for k in range(4, 12)]
    to_sib = [link(dt.at[pl.ds(al((other * 4 + rem4(x + r)) * NR), NR)], dr.at[rem4(x + r)], sib) for r in NEAR]

    def step(k, carry):
        slot = lax.rem(k, 2)
        for cp in loads(k):
            cp.wait()

        @pl.when(k < 15)
        def _():
            for cp in loads(k + 1):
                cp.start()

        for i in range(4):
            @pl.when(k == i + 8)
            def _(i=i):
                got(de.at[i + 8], stage1[i])
        cid = block_id(k)
        for n in range(NT):
            grads(slot, n, cid)
            de[k] += mm(dzb[n % 2], tb[n * TT:(n + 1) * TT, :])
            dt[n * TT:(n + 1) * TT, :] += mm(dzb[n % 2], eb[slot], TN)
        for cols in cuts(d.CL):
            tot = jnp.broadcast_to(jnp.sum(dacc[cols, :].T, **ROWS), (16, LANES))
            vb[:16, cols] = jnp.where(row16 == cid, tot, vb[:16, cols])
        for i in range(12):
            @pl.when(k == i)
            def _(i=i):
                listed[stage1[i]].start()

        return carry

    lax.fori_loop(0, 16, step, 0)
    for i in to_sib:
        listed[i].start()
    vb[16:, :] = jnp.broadcast_to(ce, (GB, d.CL))
    vby[yc] = vb[...]
    ids_vy = share(vby, yc, at_y)

    flows = {}
    keep = []

    def copy_out(src, dst):
        keep.append(pltpu.make_async_copy(src, dst, osem.at[len(keep)]))
        keep[-1].start()

    def flow_b():
        yield
        vbz[zc] = shared(vby, yc, ids_vy)
        ids = share(vbz, zc, at_z)
        yield
        dbo_out[...] = shared(vbz, zc, ids)

    def orow(rp, rq, h=ALL):
        return spot(de_out, (rem4(p + rp) * 4 + rem4(q + rq)) * BLK, BLK, h)

    def own(r, h=ALL):
        b = rem4(q + r)
        side = b // 2
        head = first_of[0] + side * (first_of[1] - first_of[0])
        blk = de.at[12 + side + jnp.where(b == head, 0, 2)]
        return blk if h is ALL else half(blk, h)

    def scatter_rest(blk, a, b, m, pp, at, ids):
        yield
        got(a, ids[0])
        add(blk(1, 0), [a])
        ids.append(send(blk(1, 0), half(m, 0), at(1)))
        yield
        got(b, ids[1])
        add(blk(3, 1), [b])
        ids.append(send(blk(3, 1), half(pp, 1), at(3)))

    def scatter_end(m, pp, ids):
        got(half(m, 1), ids[2])
        got(half(pp, 0), ids[3])
        got(half(m, 0), ids[4])
        got(half(pp, 1), ids[5])

    def far(blk, a, b, at):
        return [send(blk(2, 0), a, at(1)), send(blk(2, 1), b, at(3))]

    def near(blk, m, pp, at):
        return [send(blk(1, 1), half(m, 1), at(1)), send(blk(3, 0), half(pp, 0), at(3))]

    def both(src, dst, at):
        return [send(src, dst, at(1)), send(src, dst, at(3))]

    def relay(j):
        ids = both(orow(0, j) if j else own(0), orow(0, j), at_p)
        for r, h in ((3, 0), (1, 1)):
            yield
            got(orow(r, j), ids[h])
            ids.append(send(orow(r, j, h), orow(r, j, h), at_p(1 + 2 * h)))
        yield
        for h in (0, 1):
            got(orow(2, j, h), ids[2 + h])

    def begin(name, gen):
        flows[name] = gen
        return next(gen)

    def flow_p():
        yield
        for k, i in ((4, 13), (5, 12), (6, 15), (7, 14)):
            buf = (fp if k % 2 else fm).at[(k - 4) // 2]
            got(buf, stage1[k])
            add(de.at[i], [buf])
        yield
        for k in (8, 9):
            buf = (fp if k % 2 else fm).at[2]
            got(buf, stage1[k])
            add(de.at[k + 4], [buf])
        ids = far(own, r2a, r2b, at_q)
        yield
        for k in (10, 11):
            buf = (fp if k % 2 else fm).at[3]
            got(buf, stage1[k])
            add(de.at[k + 4], [buf])
        ids += near(own, f2m, f2p, at_q)
        yield from scatter_rest(own, r2a, r2b, f2m, f2p, at_q, ids)
        yield
        scatter_end(f2m, f2p, ids)
        fin = own(0)
        add(fin, [f2m, f2p])
        ids = both(fin, orow(0, 0), at_q)
        copy_out(fin, orow(0, 0))
        begin("0", relay(0))
        for r, h in ((3, 0), (1, 1)):
            yield
            got(orow(0, r), ids[h])
            ids.append(send(orow(0, r, h), orow(0, r, h), at_q(1 + 2 * h)))
            begin("12"[h], relay(r))
        yield
        for h in (0, 1):
            got(orow(0, 2, h), ids[2 + h])
        begin("3", relay(2))

    def xrow(r, h=ALL):
        return spot(dt, (core * 4 + rem4(x + r)) * NR, NR, h)

    def rows_out(out, n):
        def at(c):
            return lambda r, h=ALL: spot(out, (c * 4 + rem4(x + r)) * n, n, h)

        return at(core), at(other)

    def gather_x(src, out, n):
        mine, its = rows_out(out, n)
        ids = both(src, mine(0), at_x)
        sibs = [send(src, mine(0), sib)]
        copy_out(src, mine(0))
        for r, h in ((3, 0), (1, 1)):
            yield
            got(mine(r), ids[h])
            ids.append(send(mine(r, h), mine(r, h), at_x(1 + 2 * h)))
            sibs.append(send(mine(r), mine(r), sib))
        yield
        for h in (0, 1):
            got(mine(2, h), ids[2 + h])
        sibs.append(send(mine(2), mine(2), sib))
        yield
        for r, i in zip((0, 3, 1, 2), sibs):
            got(its(r), i)

    def flow_x():
        def take(*ks):
            for k in ks:
                r = NEAR[k]
                got(dr.at[rem4(x + r)], to_sib[k])
                add(xrow(r), [dr.at[rem4(x + r)]])

        yield
        take(0)
        ids = far(xrow, xa, xb, at_x)
        yield
        take(1, 2)
        ids += near(xrow, xm, xp, at_x)
        yield
        take(3)
        h_load.wait()
        ub[...] = mm(hown[...], wt_ref[...]) + row_of(bt_ref)
        yield from scatter_rest(xrow, xa, xb, xm, xp, at_x, ids)
        yield
        scatter_end(xm, xp, ids)
        layer_back()
        for i in to_sib:
            listed[i].wait_send()
        dwt = dt.at[pl.ds(al(other * HN), D)]
        for cols in cuts(D):
            dwt[:, cols] = mm(hown[...], dub[:, cols], TN)
        i_wr = send(dwt.at[pl.ds(al(other * HD), HD)], wr, sib)
        vect[tp] = jnp.concatenate([jnp.sum(vec[i], **ROWS) for i in range(GB)], axis=0)
        ids = [send(vect.at[tp], vect.at[tp], at_t(r)) for r in range(1, 8)]
        begin("w", flow_w(dwt, i_wr))
        begin("v", flow_v(ids))
        for cols in cuts(D):
            ub[:, cols] = mm(dub[...], wt_ref[cols, :], NTR).astype(BF16).astype(F32)

    lb = 64 if NR % 64 == 0 else 16

    def layer_back():
        dtown = xrow(0)
        gamma = row_of(gm_ref)
        vec[...] = jnp.zeros_like(vec)

        def back(i, carry):
            rows = pl.ds(al(i * lb, 16), lb)
            u = ub[rows, :]
            cdf = 0.5 * (1.0 + lax.erf(u * RSQRT2))
            a = u * cdf
            ctr = a - jnp.mean(a, **COLS)
            rstd = lax.rsqrt(jnp.mean(ctr * ctr, **COLS) + LN_EPS)
            xh = ctr * rstd
            g = dtown[rows, :] + xm[rows, :] + xp[rows, :]
            gx = g * xh
            gg = g * gamma
            m1 = jnp.mean(gg, **COLS)
            m2 = jnp.mean(gg * xh, **COLS)
            da = rstd * (gg - m1 - xh * m2)
            pdf = jnp.exp(u * u * -0.5) * 0.3989422804014327
            du = da * (cdf + u * pdf)
            dub[rows, :] = du.astype(BF16)
            for j, v in enumerate((gx, g, du)):
                vec[j] += jnp.sum(v.reshape(lb // GB, GB, D), axis=0)
            return carry

        lax.fori_loop(0, NR // lb, back, 0)

    def swapped(src, dst, value):
        src[...] = value
        return send(src, dst, sib)

    def flow_w(dwt, i_wr):
        def wrow(r, h=ALL):
            return spot(dwt, core * HD + rem4(x + r) * WR, WR, h)

        def piece(ref, k):
            return ref.at[pl.ds(al(k * WP), WP)]

        yield
        got(wr, i_wr)
        add(dwt.at[pl.ds(al(core * HD), HD)], [wr])
        ids = far(wrow, wxa, wxb, at_x) + near(wrow, wxm, wxp, at_x)
        yield from scatter_rest(wrow, wxa, wxb, wxm, wxp, at_x, ids)
        begin("h", gather_x(ub, dh_out, NR))
        yield
        scatter_end(wxm, wxp, ids)
        mine = wrow(0)
        add(mine, [wxm, wxp])
        ids = [send(piece(mine, rem4(q + r)), wq.at[q], at_q(r)) for r in RING]
        wq[q] = piece(mine, q)[...]
        yield
        i = swapped(w1, w2, shared(wq, q, ids))
        yield
        got(w2, i)
        wp[q] = w2[...]
        ids = share(wp, q, at_q)
        yield
        i = swapped(w3, w4, shared(wp, q, ids))
        yield
        got(w4, i)
        piece(wag, q)[...] = w4[...]
        ids = [send(piece(wag, q), piece(wag, q), at_q(r)) for r in RING]
        yield
        for r, i in zip(RING, ids):
            got(piece(wag, rem4(q - r)), i)
        yield from gather_x(wag, dwt_out, WR)

    def flow_v(ids):
        yield
        for r, i in zip(range(1, 8), ids):
            got(vect.at[rem8(tp - r)], i)
        vecq[q] = sum(vect[k] for k in range(8))
        ids = share(vecq, q, at_q)
        yield
        i = swapped(v1, v2, shared(vecq, q, ids))
        yield
        got(v2, i)
        vecp[q] = v2[...]
        ids = share(vecp, q, at_q)
        yield
        total = shared(vecp, q, ids)
        i = swapped(v3, v4, total)
        yield
        got(v4, i)
        vec_out[...] = jnp.where(core == 0, v3[...], v4[...])

    for name, gen in (("p", flow_p()), ("x", flow_x()), ("b", flow_b())):
        begin(name, gen)
    for name in STEPS:
        next(flows[name], 0)
    for gen in flows.values():
        assert next(gen, ALL) is ALL and gen.gi_frame is ALL

    for cp in keep:
        cp.wait()
    for i, cp in enumerate(listed):
        if i not in to_sib:
            cp.wait_send()


def train(d, t, h, z, meta, e, w_t, bt, gm, be):
    any_ = pl.BlockSpec(memory_space=pl.ANY)
    vm = pl.BlockSpec(memory_space=pltpu.VMEM)
    sd = jax.ShapeDtypeStruct
    D, BLK, TT, NR, WR = d.D, d.BLK, d.TT, d.NR, d.WR

    def vf(*shape):
        return pltpu.VMEM((*shape, D), F32)

    def vl(*shape):
        return pltpu.VMEM(shape, F32)

    def vh(*shape):
        return pltpu.VMEM(shape, BF16)

    def twice(v):
        return [v, v]

    dma = pltpu.SemaphoreType.DMA
    return pl.pallas_call(
        functools.partial(train_kernel, d),
        out_shape=(sd((d.VP, D), F32), sd((d.N, D), F32), sd((D, D), F32), sd((GB, D), F32), sd((3 * GB, d.CL), F32)),
        in_specs=[any_, any_, any_, vm, any_, vm, vm, vm, vm],
        out_specs=(any_, any_, any_, vm, vm),
        scratch_shapes=[
            vh(d.N, D), vh(2, BLK, D), vl(2, NT, BLK, TT), vh(2, BLK, TT), vf(d.N), vf(16, BLK), *twice(vf(4, BLK)),
            *twice(vf(d.HB)), *twice(vf(BLK)), vf(4, NR), *twice(vf(d.HR)), *twice(vf(NR)),
            vf(NR), *twice(vh(NR, D)), vf(d.HD), *twice(vf(WR // 2)), *twice(vf(WR)), *twice(vf(4, d.WP)), *twice(vf(d.WP)), *twice(vf(d.WP)), vf(WR),
            vl(8, NT, 8, TT), vl(NT, 8, TT), vl(d.CL, LANES), vl(3 * GB, d.CL), *twice(vl(4, 3 * GB, d.CL)),
            *twice(vl(4, GB, LANES)), *twice(vf(GB, GB)), *twice(vf(4, GB)), *twice(vf(GB)), *twice(vf(GB)),
            dma((2,)), dma((2,)), dma((2, NT)), dma((3,)), *twice(dma((NSEM,))),
        ],
        compiler_params=pltpu.CompilerParams(vmem_limit_bytes=VMEM_MAX, collective_id=0, has_side_effects=True),
        name="mlm_train",
    )(t, h, z, meta, e, w_t, bt, gm, be)


def finish_kernel(d, cnt_hbm, col_hbm, dh_hbm, de_hbm, dwt_hbm, vec_ref, dbo_ref,
                  dH, dE, dW, g_out, b_out, t_out, loss,
                  cnt, colb, dhb, stage, wstage, outb, isem, osem, dsem, esem, ssem):
    rows_g = GB * d.L
    src_iota = lax.broadcasted_iota(I32, (d.S, rows_g), 1)
    r_iota = lax.broadcasted_iota(I32, (d.S, 1), 0)
    first = pltpu.make_async_copy(cnt_hbm, cnt, ssem.at[0])
    first.start()
    parts = [(c * d.CH, min(d.CH, d.V - c * d.CH)) for c in range(NCH)]
    ins = [pltpu.make_async_copy(de_hbm.at[pl.ds(r, n)], stage.at[pl.ds(r, n)], dsem.at[i])
           for i, (r, n) in enumerate(parts)]
    outs = [pltpu.make_async_copy(stage.at[pl.ds(r, n)], dE.at[pl.ds(r, n)], esem.at[i])
            for i, (r, n) in enumerate(parts)]
    ins.append(pltpu.make_async_copy(dwt_hbm, wstage, dsem.at[NCH]))
    outs.append(pltpu.make_async_copy(wstage, dW, esem.at[NCH]))

    rows_h = [pltpu.make_async_copy(dh_hbm.at[pl.ds(c * d.NR, d.NR)], dhb.at[pl.ds(c * d.NR, d.NR)], isem.at[c])
              for c in range(NCH)]
    rows_h.append(pltpu.make_async_copy(col_hbm, colb, isem.at[NCH]))

    def out_copy(g, slot):
        return pltpu.make_async_copy(outb.at[slot], dH.at[pl.ds(g * rows_g, rows_g)], osem.at[slot])

    for cp in rows_h[NCH:] + rows_h[:2] + ins[:2] + rows_h[2:NCH] + ins[2:]:
        cp.start()
    for row, ref in ((LAB, g_out), (LIVE, b_out), (SRC, t_out)):
        for i, cols in enumerate(cuts(d.D)):
            ref[slice(i, i + 1), :] = vec_ref[row, cols]
    loss[...] = dbo_ref[16:17, LAB]
    first.wait()
    rows_h[NCH].wait()

    def group(g, o):
        oslot = lax.rem(g, NBUF)
        c = cnt[0, g * GB]
        for j in range(1, GB):
            c = c + cnt[0, g * GB + j]
        o = pl.multiple_of(o, 16)
        for i in range(NCH):
            @pl.when(g == i * (d.G // NCH))
            def _(i=i):
                rows_h[i].wait()

        @pl.when(g >= NBUF)
        def _():
            out_copy(g - NBUF, oslot).wait()

        src = jnp.where(r_iota < c, colb[pl.ds(o, d.S), SRC].astype(I32), -1)
        hot = (src_iota == src).astype(BF16)
        outb[oslot] = mm(hot, dhb[pl.ds(o, d.S), :].astype(BF16), TN).astype(BF16)
        out_copy(g, oslot).start()

        for i, (a, b) in enumerate(zip(ins, outs)):
            @pl.when(g == min(i, d.G - 1))
            def _(a=a, b=b):
                a.wait()
                b.start()

        return o + ((c + 15) // 16) * 16

    lax.fori_loop(0, d.G, group, jnp.int32(0))
    for g in range(d.G - NBUF, d.G):
        out_copy(g, g % NBUF).wait()
    for cp in outs:
        cp.wait()


def finish(d, cnt, col, dh, de, dwt, vec, dbo):
    any_ = pl.BlockSpec(memory_space=pl.ANY)
    vm = pl.BlockSpec(memory_space=pltpu.VMEM)
    sd = jax.ShapeDtypeStruct
    dma = pltpu.SemaphoreType.DMA
    row = sd((d.D // LANES, LANES), F32)
    return pl.pallas_call(
        functools.partial(finish_kernel, d),
        out_shape=(sd((d.B * d.L, d.D), BF16), sd((d.V, d.D), F32), sd((d.D, d.D), F32), row, row, row, sd((1, 1), F32)),
        in_specs=[any_, any_, any_, any_, any_, vm, vm],
        out_specs=(any_, any_, any_, vm, vm, vm, vm),
        scratch_shapes=[
            pltpu.SMEM((GB, d.B), I32), pltpu.VMEM((d.N, LANES), F32), pltpu.VMEM((d.N, d.D), F32),
            pltpu.VMEM((d.VP, d.D), F32), pltpu.VMEM((d.D, d.D), F32), pltpu.VMEM((NBUF, GB * d.L, d.D), BF16),
            dma((NCH + 1,)), dma((NBUF,)), dma((NCH + 1,)), dma((NCH + 1,)), dma((1,)),
        ],
        compiler_params=pltpu.CompilerParams(vmem_limit_bytes=VMEM_MAX),
        name="mlm_finish",
    )(cnt, col, dh, de, dwt, vec, dbo)


def solution(mesh):
    def step(hidden, positions, labels, weights, w_t, b_t, gamma, beta, embed, out_bias):
        d = Dims(hidden.shape, positions.shape, embed.shape)
        bias = jnp.pad(out_bias, (0, d.VP - d.V), constant_values=PAD_BIAS).reshape(-1, LANES)
        bt, gm, be = (v.reshape(-1, LANES) for v in (b_t, gamma, beta))
        h, t, z, meta, col, e, cnt = forward(d, hidden.reshape(-1, d.D), positions.T, labels.T, weights.T,
                                             w_t, bt, gm, be, embed, bias)
        de, dh, dwt, vec, dbo = train(d, t, h, z, meta, e, w_t, bt, gm, be)
        d_hidden, d_embed, d_w, d_gamma, d_beta, d_bt, loss = finish(d, cnt, col, dh, de, dwt, vec, dbo)
        d_bias = dbo[:16, :d.BLK].reshape(-1)[:d.V]
        return (loss.reshape(()), d_hidden.reshape(hidden.shape), d_w, d_bt.reshape(-1), d_gamma.reshape(-1),
                d_beta.reshape(-1), d_embed, d_bias)

    rows, vocab, whole = P("dp"), P("tp"), P()
    return jax.shard_map(step, mesh=mesh, check_vma=False,
                         in_specs=(rows, rows, rows, rows, whole, whole, whole, whole, vocab, vocab),
                         out_specs=(whole, rows, whole, whole, whole, whole, vocab, vocab))
```

```python
import functools

import jax
import jax.numpy as jnp
from jax import lax
from jax.experimental import pallas as pl
from jax.experimental.pallas import tpu as pltpu
from jax.sharding import PartitionSpec as P

F32 = jnp.float32
BF16 = jnp.bfloat16
I32 = jnp.int32
LN_EPS = 1e-12
LOSS_EPS = 1e-5
RSQRT2 = 0.7071067811865476
PAD_BIAS = -3e38
GB = 8
NT = 5
NBUF = 4
VMEM_MAX = 67043328
NCH = 8
NN = (((1,), (0,)), ((), ()))
NTR = (((1,), (1,)), ((), ()))
TN = (((0,), (0,)), ((), ()))


def mm(a, b, dims=NN):
    return lax.dot_general(a, b, dims, preferred_element_type=F32)


LANES = 128
ALL = None
ROWS, COLS = ({"axis": i, "keepdims": True} for i in range(2))
LAB, LIVE, SRC, MAX, SUM, TGT = (slice(i, i + 1) for i in range(6))


class Dims:
    def __init__(self, hidden, positions, embed):
        self.B, self.L, self.D = hidden
        self.P = positions[1]
        self.V = embed[0]
        self.G = self.B // GB
        self.S = GB * self.P
        self.N = self.B * self.P
        self.TT = self.N // NT
        self.BLK = -(-self.V // LANES) * GB
        self.VP = 16 * self.BLK
        self.CH = 2 * self.BLK
        self.NR = self.N // 8
        self.HN, self.HD, self.HB, self.HR = self.N // 2, self.D // 2, self.BLK // 2, self.NR // 2
        self.WR = self.D // 8
        self.WP = self.WR // 4
        self.CL = -(-self.BLK // LANES) * LANES


def up16(n):
    return (n + 15) // 16 * 16


def cuts(n):
    return [slice(i, min(i + LANES, n)) for i in range(0, n, LANES)]


def row_of(ref):
    return jnp.concatenate([ref[slice(i, i + 1), :] for i in range(ref.shape[0])], axis=1)


def forward_kernel(d, h_hbm, idx_ref, lab_ref, w_ref, wt_ref, bt_ref, gm_ref, be_ref, e_hbm, bias_ref,
                   h_out, t_out, z_out, meta_out, col_out, cnt_out,
                   hin, hb, tb, ub, eb, bcol, zb, col, meta, keys, cntv, cnt, par3, hot_a, hot_b, hsem, esem, zsem, tsem, osem):
    rows_g = GB * d.L
    tail = d.V - (NCH - 1) * d.CH

    def h_copy(g, slot):
        return pltpu.make_async_copy(h_hbm.at[pl.ds(g * rows_g, rows_g)], hin.at[slot], hsem.at[slot])

    def e_copy(c):
        n = d.CH if c < NCH - 1 else tail
        return pltpu.make_async_copy(e_hbm.at[pl.ds(c * d.CH, n)], eb.at[pl.ds(c * d.CH, n)], esem.at[c])

    for g in range(NBUF):
        h_copy(g, g).start()

    cntv[...] = jnp.broadcast_to(jnp.sum(w_ref[...], **ROWS), cntv.shape).astype(I32)
    to_smem = pltpu.make_async_copy(cntv, cnt, osem.at[0])
    to_smem.start()
    tp = lax.axis_index("tp")
    mine = pl.ds(pl.multiple_of((lax.rem(tp, 2) * 4 + tp // 2) * d.NR, 16), d.NR)
    pairs = (cntv, cnt_out), (hb.at[mine], h_out), (col, col_out), (meta, meta_out)
    outs = [pltpu.make_async_copy(a, b, osem.at[i + 1]) for i, (a, b) in enumerate(pairs)]
    outs[0].start()

    key = lab_ref[...] * 2048 + idx_ref[...] + 1
    keys[...] = jnp.concatenate([key, jnp.zeros((LANES - d.P, d.B), I32)], axis=0).T
    for i, ref in enumerate((bt_ref, gm_ref, be_ref)):
        par3[slice(i, i + 1), :] = row_of(ref)
    hb[...] = jnp.zeros_like(hb)
    tb[...] = jnp.zeros_like(tb)
    col[...] = jnp.zeros_like(col)
    if tail < d.CH:
        eb[d.V:, :] = jnp.zeros((d.VP - d.V, d.D), BF16)
    one_row = lax.broadcasted_iota(I32, (8, d.TT), 0) == 4
    for n in range(NT):
        meta[n] = jnp.where(one_row, 1.0, 0.0)
    for i, rows in enumerate(cuts(d.VP)):
        bcol[rows, :] = jnp.broadcast_to(bias_ref[slice(i, i + 1), :], (LANES, LANES)).T
    to_smem.wait()

    lane = lax.broadcasted_iota(I32, (1, LANES), 1)
    r_iota = lax.broadcasted_iota(I32, (d.S, LANES), 0)
    p_iota = lax.broadcasted_iota(I32, (1, LANES), 1)
    src_iota = lax.broadcasted_iota(I32, (d.S, rows_g), 1)

    def pick(g, hot):
        off = jnp.int32(0)
        key = jnp.zeros((d.S, LANES), I32)
        for j in range(GB):
            b = g * GB + j
            n_j = cnt[0, b]
            rank = jnp.where(p_iota < n_j, p_iota + off, -1)
            key = key + jnp.where(r_iota == rank, keys[pl.ds(b, 1), :] + j * d.L, 0)
            off = off + n_j
        src = jnp.sum((key & 2047).astype(F32), **COLS)
        lab = jnp.sum((key >> 11).astype(F32), **COLS)
        hot[...] = (src_iota == src.astype(I32) - 1).astype(BF16)
        live = (src > 0).astype(F32)
        return off, jnp.where(lane == 0, lab, jnp.where(lane == 1, live, src - 1))

    def pair(i, carry):
        o, n, cols = carry

        @pl.when(i == 1)
        def _():
            for c in range(NCH):
                e_copy(c).start()

        for k, (hot, nxt) in enumerate(((hot_a, hot_b), (hot_b, hot_a))):
            g = 2 * i + k
            slot = lax.rem(g, NBUF)
            h_copy(g, slot).wait()
            o = pl.multiple_of(o, 16)
            hb[pl.ds(o, d.S), :] = mm(hot[...], hin[slot]).astype(BF16)
            col[pl.ds(o, d.S), :] = cols
            o = o + up16(n)
            n, cols = pick(jnp.minimum(g + 1, d.G - 1), nxt)

            @pl.when(g + NBUF < d.G)
            def _():
                h_copy(g + NBUF, slot).start()

        return o, n, cols

    used, _, _ = lax.fori_loop(0, d.G // 2, pair, (jnp.int32(0), *pick(0, hot_a)))
    tiles = (used + d.TT - 1) // d.TT
    for cp in outs[1:3]:
        cp.start()
    for c in range(NCH):
        e_copy(c).wait()

    base_v = tp * d.V
    sub = lax.broadcasted_iota(I32, (GB, LANES), 0)
    rb = min(LANES, d.TT)
    reps = d.TT // LANES

    def z_copy(n, c):
        par = lax.rem(n, 2)
        return pltpu.make_async_copy(zb.at[par, c], z_out.at[n, pl.ds(c * d.CH, d.CH)], zsem.at[par, c])

    def t_copy(n):
        rows = pl.ds(pl.multiple_of(n * d.TT, d.TT), d.TT)
        return pltpu.make_async_copy(tb.at[rows], t_out.at[rows], tsem.at[n])

    def dense(n):
        ub[...] = mm(hb[pl.ds(pl.multiple_of(n * d.TT, d.TT), d.TT), :], wt_ref[...]) + par3[LAB, :]

    def norm(n, i):
        u = ub[i * rb:(i + 1) * rb, :]
        a = 0.5 * u * (1 + lax.erf(u * RSQRT2))
        ctr = a - jnp.mean(a, **COLS)
        var = jnp.mean(ctr * ctr, **COLS)
        t = ctr * lax.rsqrt(var + LN_EPS) * par3[LIVE, :] + par3[SRC, :]
        tb[pl.ds(pl.multiple_of(n * d.TT + i * rb, rb), rb), :] = t.astype(BF16)

    def wide(v):
        return jnp.concatenate([v] * reps, axis=1)

    def product(n, c):
        rows = slice(c * d.CH, (c + 1) * d.CH)
        t_n = tb[pl.ds(pl.multiple_of(n * d.TT, d.TT), d.TT), :]
        z = mm(eb[rows, :], t_n, NTR) + wide(bcol[rows, :])
        zb[lax.rem(n, 2), c] = z
        mx = jnp.max(z.reshape(d.CH // GB, GB, d.TT), axis=0)
        return jnp.broadcast_to(jnp.max(mx, **ROWS), (GB, d.TT))

    def tile(n, carry):
        par = lax.rem(n, 2)
        base = pl.multiple_of(n * d.TT, d.TT)
        after = jnp.minimum(n + 1, NT - 1)
        t_copy(n).start()

        @pl.when(n >= 2)
        def _():
            for c in range(NCH):
                z_copy(n, c).wait()

        for cols in cuts(d.TT):
            blk = col[pl.ds(base + cols.start, LANES), :].T
            meta[n, :3, cols] = blk[:3, :]
        lab = meta[n, LAB, :].astype(I32) - base_v
        lab8 = jnp.broadcast_to(jnp.where(lab < d.V, lab, -1), (GB, d.TT))
        m8 = jnp.full((GB, d.TT), -jnp.inf, F32)
        s8 = jnp.zeros((GB, d.TT), F32)
        t8 = jnp.zeros((GB, d.TT), F32)
        nxt = product(n, 0)
        dense(after)
        for c in range(NCH):
            z_copy(n, c).start()
            mx = jnp.maximum(m8, nxt)
            if c + 1 < NCH:
                nxt = product(n, c + 1)
            s8 = s8 * jnp.exp(m8 - mx)
            m8 = mx
            zz = zb[par, c].reshape(d.CH // GB, GB, d.TT)
            s8 = s8 + jnp.sum(jnp.exp(zz - m8[None]), axis=0)
            at = lax.broadcasted_iota(I32, zz.shape, 0) * GB + lax.broadcasted_iota(I32, zz.shape, 1) + c * d.CH
            t8 = t8 + jnp.sum(jnp.where(at == lab8[None], zz, 0.0), axis=0)
            if c >= 4 and c - 4 < d.TT // rb:
                norm(after, c - 4)
        meta[n, MAX, :] = m8[LAB, :]
        meta[n, SUM, :] = jnp.sum(s8, **ROWS)
        meta[n, TGT, :] = jnp.sum(t8, **ROWS)
        return carry

    dense(0)
    for i in range(d.TT // rb):
        norm(0, i)
    lax.fori_loop(0, tiles, tile, 0)
    outs[3].start()

    def rest(n, carry):
        t_copy(n).start()
        return carry

    lax.fori_loop(tiles, NT, rest, 0)
    def drain(n, carry):
        for c in range(NCH):
            z_copy(n, c).wait()
        return carry

    lax.fori_loop(jnp.maximum(tiles - 2, 0), tiles, drain, 0)

    for n in range(NT):
        t_copy(n).wait()
    for cp in outs:
        cp.wait()


def forward(d, h2, idx, lab, w, w_t, bt, gm, be, embed, bias):
    any_ = pl.BlockSpec(memory_space=pl.ANY)
    vm = pl.BlockSpec(memory_space=pltpu.VMEM)
    sd = jax.ShapeDtypeStruct
    dma = pltpu.SemaphoreType.DMA
    return pl.pallas_call(
        functools.partial(forward_kernel, d),
        out_shape=(sd((d.NR, d.D), BF16), sd((d.N, d.D), BF16), sd((NT, d.VP, d.TT), F32), sd((NT, 8, d.TT), F32),
                   sd((d.N, LANES), F32), sd((8, d.B), I32)),
        in_specs=[any_, vm, vm, vm, vm, vm, vm, vm, any_, vm],
        out_specs=(any_,) * 6,
        scratch_shapes=[
            pltpu.VMEM((NBUF, GB * d.L, d.D), BF16),
            pltpu.VMEM((d.N, d.D), BF16),
            pltpu.VMEM((d.N, d.D), BF16),
            pltpu.VMEM((d.TT, d.D), F32),
            pltpu.VMEM((d.VP, d.D), BF16),
            pltpu.VMEM((d.VP, LANES), F32),
            pltpu.VMEM((2, NCH, d.CH, d.TT), F32),
            pltpu.VMEM((d.N, LANES), F32),
            pltpu.VMEM((NT, 8, d.TT), F32),
            pltpu.VMEM((d.B, LANES), I32),
            pltpu.VMEM((8, d.B), I32),
            pltpu.SMEM((8, d.B), I32),
            pltpu.VMEM((8, d.D), F32),
            pltpu.VMEM((d.S, GB * d.L), BF16),
            pltpu.VMEM((d.S, GB * d.L), BF16),
            dma((NBUF,)), dma((NCH,)), dma((2, NCH)), dma((NT,)), dma((5,)),
        ],
        compiler_params=pltpu.CompilerParams(vmem_limit_bytes=VMEM_MAX),
        name="mlm_forward",
    )(h2, idx, lab, w, w_t, bt, gm, be, embed, bias)


MESH = pl.DeviceIdType.MESH
RING = (1, 2, 3)
OTHERS = range(1, 8)
NSEM = 128
NEAR = (2, 1, 3, 0)
CODES = "200210201211110300111301100310101311000010001011"
ORDER = [tuple(int(c) for c in CODES[i:i + 3]) for i in range(0, len(CODES), 3)]
STEPS = "pxxxpxxpppbpbxwvpp00wwvvwpvvww11ww22hhw033h1hww23ww"


def train_kernel(d, t_hbm, h_hbm, z_hbm, meta, e_hbm, wt_ref, bt_ref, gm_ref, be_ref,
                 de_out, dh_out, dwt_out, vec_out, dbo_out,
                 tb, eb, zb, dzb, dt, de, fm, fp, r2a, r2b, f2m, f2p, dr, xa, xb, xm, xp,
                 ub, dub, hown, wr, wxa, wxb, wxm, wxp, wq, wp, w1, w2, w3, w4, wag, srecv, comb, dacc, vb, vby, vbz,
                 dnp, dnq, vec, vect, vecp, vecq, v1, v2, v3, v4, lsem, esem, zsem, osem, ss, rs):
    dp = lax.axis_index("dp")
    tp = lax.axis_index("tp")
    zc, yc = dp // 4, lax.rem(dp, 4)
    x, core = tp // 2, lax.rem(tp, 2)
    other = 1 - core
    pm, qm = 1 + 3 * core, 4 - 3 * core
    p = yc + core * (zc - yc)
    q = zc + core * (yc - zc)
    D, BLK, TT, NR = d.D, d.BLK, d.TT, d.NR
    HN, HD, WR, WP = d.HN, d.HD, d.WR, d.WP

    def rem4(v):
        return lax.rem(v + 4, 4)

    def rem8(v):
        return lax.rem(v + 8, 8)

    def at_p(r):
        return {"dp": rem4(p + r) * pm + q * qm}

    def at_q(r):
        return {"dp": p * pm + rem4(q + r) * qm}

    def at_y(r):
        return {"dp": zc * 4 + rem4(yc + r)}

    def at_z(r):
        return {"dp": rem4(zc + r) * 4 + yc}

    def at_x(r):
        return {"tp": rem4(x + r) * 2 + core}

    def at_t(r):
        return {"tp": rem8(tp + r)}

    sib = {"tp": x * 2 + other}

    def al(v, m=8):
        return pl.multiple_of(v, m)

    listed = []

    def link(src, dst, dev):
        i = len(listed)
        listed.append(pltpu.make_async_remote_copy(src_ref=src, dst_ref=dst, send_sem=ss.at[i], recv_sem=rs.at[i],
                                                   device_id=dev, device_id_type=MESH))
        return i

    def send(src, dst, dev):
        i = link(src, dst, dev)
        listed[i].start()
        return i

    def got(dst, i):
        pltpu.make_async_remote_copy(src_ref=dst, dst_ref=dst, send_sem=ss.at[i], recv_sem=rs.at[i],
                                     device_id=sib, device_id_type=MESH).wait_recv()

    def share(buf, own, at):
        return [send(buf.at[own], buf.at[own], at(r)) for r in RING]

    def shared(buf, own, ids):
        for r, i in zip(RING, ids):
            got(buf.at[rem4(own - r)], i)
        return buf[0] + buf[1] + buf[2] + buf[3]

    def half(ref, h):
        n = ref.shape[0] // 2
        return ref.at[pl.ds(h * n, n)]

    def add(dst, srcs):
        nr = dst.shape[0]
        step = max(s for s in (8, 24, 40) if nr % s == 0)

        def body(i, carry):
            rows = pl.ds(al(i * step), step)
            v = dst[rows, :]
            for s in srcs:
                v = v + s[rows, :]
            dst[rows, :] = v
            return carry

        lax.fori_loop(0, nr // step, body, 0)

    def spot(ref, base, n, h=ALL):
        if h is ALL:
            return ref.at[pl.ds(al(base), n)]
        return ref.at[pl.ds(al(base + h * (n // 2)), n // 2)]

    first_of = (jnp.where((q == 1) | (q == 2), 0, 1), jnp.where((q == 1) | (q == 2), 3, 2))

    def block_id(k):
        out = p * 0
        for i, (rel, h, second) in enumerate(ORDER):
            b = 4 * h + 1 - first_of[h] if second else first_of[h]
            out = jnp.where(k == i, rem4(p + rel) * 4 + b, out)
        return out

    last = d.VP // BLK - 1
    tail = d.V - last * BLK

    def loads(k, act):
        slot = lax.rem(k, 2)
        b = block_id(k)
        r = b * BLK
        for n in range(NT):
            act(pltpu.make_async_copy(z_hbm.at[n, pl.ds(al(r), BLK)], zb.at[slot, n], zsem.at[slot, n]))

        @pl.when(b < last)
        def _():
            act(pltpu.make_async_copy(e_hbm.at[pl.ds(al(r, 16), BLK)], eb.at[slot], esem.at[slot]))

        @pl.when(b == last)
        def _():
            act(pltpu.make_async_copy(e_hbm.at[pl.ds(last * BLK, tail)], eb.at[slot, pl.ds(0, tail)], esem.at[slot]))

    def start(cp):
        cp.start()

    def wait(cp):
        cp.wait()

    eb[...] = jnp.zeros_like(eb)
    loads(jnp.int32(0), start)
    t_load = pltpu.make_async_copy(t_hbm, tb, lsem.at[0])
    h_load = pltpu.make_async_copy(h_hbm, hown, lsem.at[1])
    t_load.start()
    h_load.start()

    barrier = pltpu.get_barrier_semaphore()
    peers = [f(r) for f in (at_y, at_z) for r in RING] + [at_t(r) for r in OTHERS]
    for dev in peers:
        pl.semaphore_signal(barrier, inc=1, device_id=dev, device_id_type=MESH)
    wsum = jnp.zeros((1, 1), F32)
    for n in range(NT):
        wsum = wsum + jnp.sum(meta[n, LIVE, :], **COLS)
    dnp[yc] = jnp.broadcast_to(wsum, dnp.shape[1:])
    srecv[tp] = meta[...]
    pl.semaphore_wait(barrier, len(peers))

    ids_y = share(dnp, yc, at_y)
    ids_t = [send(meta, srecv.at[tp], at_t(r)) for r in OTHERS]
    dt[...] = jnp.zeros_like(dt)
    for k in (*range(8), *range(12, 16)):
        de[k] = jnp.zeros((BLK, D), F32)
    vb[...] = jnp.zeros_like(vb)
    dnq[zc] = shared(dnp, yc, ids_y)
    ids_z = share(dnq, zc, at_z)
    for r, i in zip(OTHERS, ids_t):
        got(srecv.at[rem8(tp - r)], i)
    tiles = []
    for n in range(NT):
        mx = srecv[0, n, MAX, :]
        for k in OTHERS:
            mx = jnp.maximum(mx, srecv[k, n, MAX, :])
        tot = jnp.zeros((1, TT), F32)
        tgt = jnp.zeros((1, TT), F32)
        for k in range(8):
            tot = tot + srecv[k, n, SUM, :] * jnp.exp(srecv[k, n, MAX, :] - mx)
            tgt = tgt + srecv[k, n, TGT, :]
        lab = meta[n, LAB, :] - (tp * d.V).astype(F32)
        comb[n, LAB, :] = mx
        comb[n, LIVE, :] = 1.0 / tot
        comb[n, MAX, :] = jnp.where(lab < d.V, lab, -1.0)
        tiles.append(jnp.log(tot) + mx - tgt)
    denom = shared(dnq, zc, ids_z)[LAB, LAB] + LOSS_EPS
    ce = jnp.zeros((1, TT), F32)
    for n in range(NT):
        w = meta[n, LIVE, :]
        c = w / denom
        comb[n, LIVE, :] = comb[n, LIVE, :] * c
        comb[n, SRC, :] = c
        ce = ce + w * tiles[n]
    ce = jnp.sum(ce, **COLS) / denom
    t_load.wait()

    sub = lax.broadcasted_iota(I32, (16, LANES), 0)
    row16 = lax.broadcasted_iota(I32, (16, LANES), 0)
    dacc[BLK:, :] = jnp.zeros((d.CL - BLK, LANES), F32)

    def grads(slot, n, cid):
        m8 = jnp.broadcast_to(comb[n, LAB, :], (16, TT))
        a8 = jnp.broadcast_to(comb[n, LIVE, :], (16, TT))
        c8 = jnp.broadcast_to(comb[n, SRC, :], (16, TT))
        live = c8 > 0
        l8 = jnp.broadcast_to(comb[n, MAX, :].astype(I32) - cid * BLK, (16, TT))
        for i in range(BLK // 16):
            rows = slice(i * 16, (i + 1) * 16)
            g = jnp.exp(zb[slot, n, rows, :] - m8) * a8
            at = jnp.concatenate([sub + i * 16] * (TT // LANES), axis=1)
            g = g - jnp.where(at == l8, c8, 0.0)
            if n:
                g = jnp.where(live, g, 0.0)
            dzb[n % 2, rows, :] = g.astype(BF16)
            part = sum(g[:, cols] for cols in cuts(TT))
            dacc[rows, :] = part if n == 0 else dacc[rows, :] + part

    stage1 = [link(de.at[k], de.at[k + 8], at_p(3 if k % 2 else 1)) for k in range(4)]
    stage1 += [link(de.at[k], (fp if k % 2 else fm).at[(k - 4) // 2], at_p(3 if k % 2 else 1)) for k in range(4, 12)]
    to_sib = [link(dt.at[pl.ds(al((other * 4 + rem4(x + r)) * NR), NR)], dr.at[rem4(x + r)], sib) for r in NEAR]

    def step(k, carry):
        slot = lax.rem(k, 2)
        loads(k, wait)

        @pl.when(k < 15)
        def _():
            loads(k + 1, start)

        for i in range(4):
            @pl.when(k == i + 8)
            def _(i=i):
                got(de.at[i + 8], stage1[i])
        cid = block_id(k)
        for n in range(NT):
            grads(slot, n, cid)
            de[k] += mm(dzb[n % 2], tb[n * TT:(n + 1) * TT, :])
            dt[n * TT:(n + 1) * TT, :] += mm(dzb[n % 2], eb[slot], TN)
        for cols in cuts(d.CL):
            tot = jnp.broadcast_to(jnp.sum(dacc[cols, :].T, **ROWS), (16, LANES))
            vb[:16, cols] = jnp.where(row16 == cid, tot, vb[:16, cols])
        for i in range(12):
            @pl.when(k == i)
            def _(i=i):
                listed[stage1[i]].start()

        return carry

    lax.fori_loop(0, 16, step, 0)
    for i in to_sib:
        listed[i].start()
    vb[16:, :] = jnp.broadcast_to(ce, (GB, d.CL))
    vby[yc] = vb[...]
    ids_vy = share(vby, yc, at_y)

    flows = {}
    keep = []

    def copy_out(src, dst):
        keep.append(pltpu.make_async_copy(src, dst, osem.at[len(keep)]))
        keep[-1].start()

    def flow_b():
        yield
        vbz[zc] = shared(vby, yc, ids_vy)
        ids = share(vbz, zc, at_z)
        yield
        dbo_out[...] = shared(vbz, zc, ids)

    def orow(rp, rq, h=ALL):
        return spot(de_out, (rem4(p + rp) * 4 + rem4(q + rq)) * BLK, BLK, h)

    def own(r, h=ALL):
        b = rem4(q + r)
        side = b // 2
        head = first_of[0] + side * (first_of[1] - first_of[0])
        blk = de.at[12 + side + jnp.where(b == head, 0, 2)]
        return blk if h is ALL else half(blk, h)

    def scatter_rest(blk, a, b, m, pp, at, ids):
        yield
        got(a, ids[0])
        add(blk(1, 0), [a])
        ids.append(send(blk(1, 0), half(m, 0), at(1)))
        yield
        got(b, ids[1])
        add(blk(3, 1), [b])
        ids.append(send(blk(3, 1), half(pp, 1), at(3)))

    def scatter_end(m, pp, ids):
        got(half(m, 1), ids[2])
        got(half(pp, 0), ids[3])
        got(half(m, 0), ids[4])
        got(half(pp, 1), ids[5])

    def far(blk, a, b, at):
        return [send(blk(2, 0), a, at(1)), send(blk(2, 1), b, at(3))]

    def near(blk, m, pp, at):
        return [send(blk(1, 1), half(m, 1), at(1)), send(blk(3, 0), half(pp, 0), at(3))]

    def both(src, dst, at):
        return [send(src, dst, at(1)), send(src, dst, at(3))]

    def relay(j):
        ids = both(orow(0, j) if j else own(0), orow(0, j), at_p)
        for r, h in ((3, 0), (1, 1)):
            yield
            got(orow(r, j), ids[h])
            ids.append(send(orow(r, j, h), orow(r, j, h), at_p(1 + 2 * h)))
        yield
        for h in (0, 1):
            got(orow(2, j, h), ids[2 + h])

    def begin(name, gen):
        flows[name] = gen
        return next(gen)

    def flow_p():
        yield
        for k, i in ((4, 13), (5, 12), (6, 15), (7, 14)):
            buf = (fp if k % 2 else fm).at[(k - 4) // 2]
            got(buf, stage1[k])
            add(de.at[i], [buf])
        yield
        for k in (8, 9):
            buf = (fp if k % 2 else fm).at[2]
            got(buf, stage1[k])
            add(de.at[k + 4], [buf])
        ids = far(own, r2a, r2b, at_q)
        yield
        for k in (10, 11):
            buf = (fp if k % 2 else fm).at[3]
            got(buf, stage1[k])
            add(de.at[k + 4], [buf])
        ids += near(own, f2m, f2p, at_q)
        yield from scatter_rest(own, r2a, r2b, f2m, f2p, at_q, ids)
        yield
        scatter_end(f2m, f2p, ids)
        fin = own(0)
        add(fin, [f2m, f2p])
        ids = both(fin, orow(0, 0), at_q)
        copy_out(fin, orow(0, 0))
        begin("0", relay(0))
        for r, h in ((3, 0), (1, 1)):
            yield
            got(orow(0, r), ids[h])
            ids.append(send(orow(0, r, h), orow(0, r, h), at_q(1 + 2 * h)))
            begin("12"[h], relay(r))
        yield
        for h in (0, 1):
            got(orow(0, 2, h), ids[2 + h])
        begin("3", relay(2))

    def xrow(r, h=ALL):
        return spot(dt, (core * 4 + rem4(x + r)) * NR, NR, h)

    def rows_out(out, n):
        def at(c):
            return lambda r, h=ALL: spot(out, (c * 4 + rem4(x + r)) * n, n, h)

        return at(core), at(other)

    def gather_x(src, out, n):
        mine, its = rows_out(out, n)
        ids = both(src, mine(0), at_x)
        sibs = [send(src, mine(0), sib)]
        copy_out(src, mine(0))
        for r, h in ((3, 0), (1, 1)):
            yield
            got(mine(r), ids[h])
            ids.append(send(mine(r, h), mine(r, h), at_x(1 + 2 * h)))
            sibs.append(send(mine(r), mine(r), sib))
        yield
        for h in (0, 1):
            got(mine(2, h), ids[2 + h])
        sibs.append(send(mine(2), mine(2), sib))
        yield
        for r, i in zip((0, 3, 1, 2), sibs):
            got(its(r), i)

    def flow_x():
        def take(*ks):
            for k in ks:
                r = NEAR[k]
                got(dr.at[rem4(x + r)], to_sib[k])
                add(xrow(r), [dr.at[rem4(x + r)]])

        yield
        take(0)
        ids = far(xrow, xa, xb, at_x)
        yield
        take(1, 2)
        ids += near(xrow, xm, xp, at_x)
        yield
        take(3)
        h_load.wait()
        ub[...] = mm(hown[...], wt_ref[...]) + row_of(bt_ref)
        yield from scatter_rest(xrow, xa, xb, xm, xp, at_x, ids)
        yield
        scatter_end(xm, xp, ids)
        layer_back()
        for i in to_sib:
            listed[i].wait_send()
        dwt = dt.at[pl.ds(al(other * HN), D)]
        for cols in cuts(D):
            dwt[:, cols] = mm(hown[...], dub[:, cols], TN)
        i_wr = send(dwt.at[pl.ds(al(other * HD), HD)], wr, sib)
        vect[tp] = jnp.concatenate([jnp.sum(vec[i], **ROWS) for i in range(GB)], axis=0)
        ids = [send(vect.at[tp], vect.at[tp], at_t(r)) for r in OTHERS]
        begin("w", flow_w(dwt, i_wr))
        begin("v", flow_v(ids))
        for cols in cuts(D):
            ub[:, cols] = mm(dub[...], wt_ref[cols, :], NTR).astype(BF16).astype(F32)

    lb = 64 if NR % 64 == 0 else 16

    def layer_back():
        dtown = xrow(0)
        gamma = row_of(gm_ref)
        vec[...] = jnp.zeros_like(vec)

        def back(i, carry):
            rows = pl.ds(al(i * lb, 16), lb)
            u = ub[rows, :]
            cdf = 0.5 * (1.0 + lax.erf(u * RSQRT2))
            a = u * cdf
            ctr = a - jnp.mean(a, **COLS)
            rstd = lax.rsqrt(jnp.mean(ctr * ctr, **COLS) + LN_EPS)
            xh = ctr * rstd
            g = dtown[rows, :] + xm[rows, :] + xp[rows, :]
            gx = g * xh
            gg = g * gamma
            m1 = jnp.mean(gg, **COLS)
            m2 = jnp.mean(gg * xh, **COLS)
            da = rstd * (gg - m1 - xh * m2)
            pdf = jnp.exp(u * u * -0.5) * 0.3989422804014327
            du = da * (cdf + u * pdf)
            dub[rows, :] = du.astype(BF16)
            for j, v in enumerate((gx, g, du)):
                vec[j] += jnp.sum(v.reshape(lb // GB, GB, D), axis=0)
            return carry

        lax.fori_loop(0, NR // lb, back, 0)

    def swapped(src, dst, value):
        src[...] = value
        return send(src, dst, sib)

    def flow_w(dwt, i_wr):
        def wrow(r, h=ALL):
            return spot(dwt, core * HD + rem4(x + r) * WR, WR, h)

        def piece(ref, k):
            return ref.at[pl.ds(al(k * WP), WP)]

        yield
        got(wr, i_wr)
        add(dwt.at[pl.ds(al(core * HD), HD)], [wr])
        ids = far(wrow, wxa, wxb, at_x) + near(wrow, wxm, wxp, at_x)
        yield from scatter_rest(wrow, wxa, wxb, wxm, wxp, at_x, ids)
        begin("h", gather_x(ub, dh_out, NR))
        yield
        scatter_end(wxm, wxp, ids)
        mine = wrow(0)
        add(mine, [wxm, wxp])
        ids = [send(piece(mine, rem4(q + r)), wq.at[q], at_q(r)) for r in RING]
        wq[q] = piece(mine, q)[...]
        yield
        i = swapped(w1, w2, shared(wq, q, ids))
        yield
        got(w2, i)
        wp[q] = w2[...]
        ids = share(wp, q, at_q)
        yield
        i = swapped(w3, w4, shared(wp, q, ids))
        yield
        got(w4, i)
        piece(wag, q)[...] = w4[...]
        ids = [send(piece(wag, q), piece(wag, q), at_q(r)) for r in RING]
        yield
        for r, i in zip(RING, ids):
            got(piece(wag, rem4(q - r)), i)
        yield from gather_x(wag, dwt_out, WR)

    def flow_v(ids):
        yield
        for r, i in zip(OTHERS, ids):
            got(vect.at[rem8(tp - r)], i)
        vecq[q] = sum(vect[k] for k in range(8))
        ids = share(vecq, q, at_q)
        yield
        i = swapped(v1, v2, shared(vecq, q, ids))
        yield
        got(v2, i)
        vecp[q] = v2[...]
        ids = share(vecp, q, at_q)
        yield
        total = shared(vecp, q, ids)
        i = swapped(v3, v4, total)
        yield
        got(v4, i)
        vec_out[...] = jnp.where(core == 0, v3[...], v4[...])

    for name, gen in (("p", flow_p()), ("x", flow_x()), ("b", flow_b())):
        begin(name, gen)
    for name in STEPS:
        next(flows[name], 0)
    for gen in flows.values():
        assert next(gen, ALL) is ALL and gen.gi_frame is ALL

    for cp in keep:
        cp.wait()
    for i, cp in enumerate(listed):
        if i not in to_sib:
            cp.wait_send()


def train(d, t, h, z, meta, e, w_t, bt, gm, be):
    any_ = pl.BlockSpec(memory_space=pl.ANY)
    vm = pl.BlockSpec(memory_space=pltpu.VMEM)
    sd = jax.ShapeDtypeStruct
    D, BLK, TT, NR, WR = d.D, d.BLK, d.TT, d.NR, d.WR

    def vf(*shape):
        return pltpu.VMEM((*shape, D), F32)

    def vl(*shape):
        return pltpu.VMEM(shape, F32)

    def vh(*shape):
        return pltpu.VMEM(shape, BF16)

    def twice(v):
        return [v, v]

    dma = pltpu.SemaphoreType.DMA
    return pl.pallas_call(
        functools.partial(train_kernel, d),
        out_shape=(sd((d.VP, D), F32), sd((d.N, D), F32), sd((D, D), F32), sd((GB, D), F32), sd((3 * GB, d.CL), F32)),
        in_specs=[any_, any_, any_, vm, any_, vm, vm, vm, vm],
        out_specs=(any_, any_, any_, vm, vm),
        scratch_shapes=[
            vh(d.N, D), vh(2, BLK, D), vl(2, NT, BLK, TT), vh(2, BLK, TT), vf(d.N), vf(16, BLK), *twice(vf(4, BLK)),
            *twice(vf(d.HB)), *twice(vf(BLK)), vf(4, NR), *twice(vf(d.HR)), *twice(vf(NR)),
            vf(NR), *twice(vh(NR, D)), vf(d.HD), *twice(vf(WR // 2)), *twice(vf(WR)), *twice(vf(4, d.WP)), *twice(vf(d.WP)), *twice(vf(d.WP)), vf(WR),
            vl(8, NT, 8, TT), vl(NT, 8, TT), vl(d.CL, LANES), vl(3 * GB, d.CL), *twice(vl(4, 3 * GB, d.CL)),
            *twice(vl(4, GB, LANES)), *twice(vf(GB, GB)), *twice(vf(4, GB)), *twice(vf(GB)), *twice(vf(GB)),
            dma((2,)), dma((2,)), dma((2, NT)), dma((3,)), *twice(dma((NSEM,))),
        ],
        compiler_params=pltpu.CompilerParams(vmem_limit_bytes=VMEM_MAX, collective_id=0, has_side_effects=True),
        name="mlm_train",
    )(t, h, z, meta, e, w_t, bt, gm, be)


def finish_kernel(d, cnt_hbm, col_hbm, dh_hbm, de_hbm, dwt_hbm, vec_ref, dbo_ref,
                  dH, dE, dW, g_out, b_out, t_out, loss,
                  cnt, colb, dhb, stage, wstage, outb, isem, osem, dsem, esem, ssem):
    rows_g = GB * d.L
    src_iota = lax.broadcasted_iota(I32, (d.S, rows_g), 1)
    r_iota = lax.broadcasted_iota(I32, (d.S, 1), 0)
    first = pltpu.make_async_copy(cnt_hbm, cnt, ssem.at[0])
    first.start()
    parts = [(c * d.CH, min(d.CH, d.V - c * d.CH)) for c in range(NCH)]
    ins = [pltpu.make_async_copy(de_hbm.at[pl.ds(r, n)], stage.at[pl.ds(r, n)], dsem.at[i])
           for i, (r, n) in enumerate(parts)]
    outs = [pltpu.make_async_copy(stage.at[pl.ds(r, n)], dE.at[pl.ds(r, n)], esem.at[i])
            for i, (r, n) in enumerate(parts)]
    ins.append(pltpu.make_async_copy(dwt_hbm, wstage, dsem.at[NCH]))
    outs.append(pltpu.make_async_copy(wstage, dW, esem.at[NCH]))

    per = d.G // NCH
    rows_h = [pltpu.make_async_copy(dh_hbm.at[pl.ds(c * d.NR, d.NR)], dhb.at[pl.ds(c * d.NR, d.NR)], isem.at[c])
              for c in range(NCH)]
    rows_c = pltpu.make_async_copy(col_hbm, colb, ssem.at[1])

    def out_copy(g, slot):
        return pltpu.make_async_copy(outb.at[slot], dH.at[pl.ds(g * rows_g, rows_g)], osem.at[slot])

    rows_c.start()
    rows_h[0].start()
    for row, ref in ((LAB, g_out), (LIVE, b_out), (SRC, t_out)):
        for i, cols in enumerate(cuts(d.D)):
            ref[slice(i, i + 1), :] = vec_ref[row, cols]
    loss[...] = dbo_ref[16:17, LAB]
    first.wait()
    rows_c.wait()

    def group(g, o):
        oslot = lax.rem(g, NBUF)
        c = cnt[0, g * GB]
        for j in range(1, GB):
            c = c + cnt[0, g * GB + j]
        o = pl.multiple_of(o, 16)
        for i in range(NCH + 1):
            @pl.when(g == min(i * per, d.G - 1))
            def _(i=i):
                if i < NCH:
                    rows_h[i].wait()
                if i + 1 < NCH:
                    rows_h[i + 1].start()
                ins[i].start()
                if i:
                    ins[i - 1].wait()
                    outs[i - 1].start()

        @pl.when(g >= NBUF)
        def _():
            out_copy(g - NBUF, oslot).wait()

        src = jnp.where(r_iota < c, colb[pl.ds(o, d.S), SRC].astype(I32), -1)
        hot = (src_iota == src).astype(BF16)
        outb[oslot] = mm(hot, dhb[pl.ds(o, d.S), :].astype(BF16), TN).astype(BF16)
        out_copy(g, oslot).start()
        return o + up16(c)

    lax.fori_loop(0, d.G, group, jnp.int32(0))
    for g in range(d.G - NBUF, d.G):
        out_copy(g, g % NBUF).wait()
    ins[NCH].wait()
    outs[NCH].start()
    for cp in outs:
        cp.wait()


def finish(d, cnt, col, dh, de, dwt, vec, dbo):
    any_ = pl.BlockSpec(memory_space=pl.ANY)
    vm = pl.BlockSpec(memory_space=pltpu.VMEM)
    sd = jax.ShapeDtypeStruct
    dma = pltpu.SemaphoreType.DMA
    row = sd((d.D // LANES, LANES), F32)
    return pl.pallas_call(
        functools.partial(finish_kernel, d),
        out_shape=(sd((d.B * d.L, d.D), BF16), sd((d.V, d.D), F32), sd((d.D, d.D), F32), row, row, row, sd((1, 1), F32)),
        in_specs=[any_, any_, any_, any_, any_, vm, vm],
        out_specs=(any_, any_, any_, vm, vm, vm, vm),
        scratch_shapes=[
            pltpu.SMEM((GB, d.B), I32), pltpu.VMEM((d.N, LANES), F32), pltpu.VMEM((d.N, d.D), F32),
            pltpu.VMEM((d.VP, d.D), F32), pltpu.VMEM((d.D, d.D), F32), pltpu.VMEM((NBUF, GB * d.L, d.D), BF16),
            dma((NCH,)), dma((NBUF,)), dma((NCH + 1,)), dma((NCH + 1,)), dma((2,)),
        ],
        compiler_params=pltpu.CompilerParams(vmem_limit_bytes=VMEM_MAX),
        name="mlm_finish",
    )(cnt, col, dh, de, dwt, vec, dbo)


def solution(mesh):
    def step(hidden, positions, labels, weights, w_t, b_t, gamma, beta, embed, out_bias):
        d = Dims(hidden.shape, positions.shape, embed.shape)
        bias = jnp.pad(out_bias, (0, d.VP - d.V), constant_values=PAD_BIAS).reshape(-1, LANES)
        bt, gm, be = (v.reshape(-1, LANES) for v in (b_t, gamma, beta))
        h, t, z, meta, col, cnt = forward(d, hidden.reshape(-1, d.D), positions.T, labels.T, weights.T,
                                             w_t, bt, gm, be, embed, bias)
        de, dh, dwt, vec, dbo = train(d, t, h, z, meta, embed, w_t, bt, gm, be)
        d_hidden, d_embed, d_w, d_gamma, d_beta, d_bt, loss = finish(d, cnt, col, dh, de, dwt, vec, dbo)
        d_bias = dbo[:16, :d.BLK].reshape(-1)[:d.V]
        return (loss.reshape(()), d_hidden.reshape(hidden.shape), d_w, d_bt.reshape(-1), d_gamma.reshape(-1),
                d_beta.reshape(-1), d_embed, d_bias)

    rows, vocab, whole = P("dp"), P("tp"), P()
    return jax.shard_map(step, mesh=mesh, check_vma=False,
                         in_specs=(rows, rows, rows, rows, whole, whole, whole, whole, vocab, vocab),
                         out_specs=(whole, rows, whole, whole, whole, whole, vocab, vocab))
```
